256 devices in a mesh: tm: 128 (over x, y_hi, z, core), chan: 2 (over y_lo).
Axes of the slice: x: 4, y: 4 (y_hi: 2, y_lo: 2; y = y_hi * 2 + y_lo), z: 8, core: 2. Of those that a mesh axis runs over, the one named last changes fastest.
Arguments:
- random_forcing: bfloat16 [49152, 4096], P('tm', 'chan'), may hold values from -6 to 6
- eigen_root_table: float32 [768, 4096], P(None, 'chan'), may hold values from 0.1 to 2
- lane_fading_speed: float32 [4096], P('chan'), may hold values from 4.0690104e-08 to 0.025, as said below
- sudden_shrink: float32 [49152], P('tm'), may hold values from 0.125 to 1, as said below
Outputs:
- sample: float32 [49152, 4096], P('tm', 'chan')
The draws below stay inside these ranges and needn't reach their ends.
Inputs may be any that keep to these rules, and one draw needn't show every extreme that they name: `lane_fading_speed`: every channel's rate is positive. `sudden_shrink`: every entry lies in (0, 1], and the product of all entries is at most 0.52.
All inputs are finite; a program needn't handle non-finite values.
Results may differ from the reference program's by a relative error of at most 0.0003.
Values may be sent and summed in bfloat16 or wider, within the bound.
A program may use at most 192 MiB of HBM per device.

```python
import math
import jax
import jax.numpy as jnp
from jax import lax

CHANNELS = 4096
BLOCK_TICKS = 384
TIME = 49152
N_TM = 128


def draw_lane_fading_speed(key, part):
    first = jax.random.fold_in(key, 0)
    lowest = 0.002 / TIME
    return jnp.exp(jnp.log(lowest) + jax.random.uniform(first, (CHANNELS,), jnp.float32) * jnp.log(0.025 / lowest)).astype(jnp.float32)


def draw_sudden_shrink(key, part):
    first, second = jax.random.split(jax.random.fold_in(key, 17), 2)
    places = jax.random.permutation(first, TIME)[:3].astype(jnp.int32)
    factors = jax.random.uniform(second, (3,), jnp.float32, 0.5, 0.8)
    positions = jnp.arange(TIME, dtype=jnp.int32)
    scaled = jnp.where(positions[None, :] == places[:, None], factors[:, None], 1.0)
    return jnp.prod(scaled, axis=0).astype(jnp.float32)


def steps_of(key, shape, cuts, least, high):
    def one(axis_at, shards_of):
        heights = jax.random.uniform(jax.random.fold_in(jax.random.fold_in(key, 6), axis_at), (shards_of,), jnp.float32, least / len(cuts), high / len(cuts))
        return jnp.repeat(jnp.exp(heights), shape[axis_at] // shards_of).reshape((-1,) + (1,) * (len(shape) - axis_at - 1))

    loudness = one(*cuts[0])
    for cut in cuts[1:]:
        loudness = loudness * one(*cut)
    return loudness


def noise(key, shape, spread, bound, cuts=(), kind=jnp.bfloat16):
    gain = steps_of(key, shape, cuts, -0.22, 0.18) if cuts else 1.0
    drawn = jax.random.normal(key, shape, jnp.float32) * spread * gain
    return jnp.minimum(jnp.maximum(drawn, -bound), bound).astype(kind)


def setup_inputs(seed: int = 0) -> dict:
    key_of = jax.random.split(jax.random.key(seed), 5)
    random_forcing = noise(key_of[0], (TIME, CHANNELS), 1.0, 6.0, ((0, 128), (1, 2)))
    eigen_root_table = jnp.clip(jnp.exp(math.log(2.0) - 2.9957323 * jax.random.uniform(key_of[1], (2 * BLOCK_TICKS, CHANNELS), jnp.float32) ** steps_of(key_of[1], (2 * BLOCK_TICKS, CHANNELS), ((1, 2),), -0.2, 0.2)), 0.1, 2.0)
    lane_fading_speed = draw_lane_fading_speed(jax.random.fold_in(key_of[4], 71), 0)
    sudden_shrink = draw_sudden_shrink(jax.random.fold_in(key_of[4], 71), 0)
    return {"random_forcing": random_forcing, "eigen_root_table": eigen_root_table, "lane_fading_speed": lane_fading_speed, "sudden_shrink": sudden_shrink}


def combine(former, latter):
    return (former[0] + latter[0], jnp.exp(latter[0]) * former[1] + latter[1])

def reference(random_forcing, eigen_root_table, lane_fading_speed, sudden_shrink):
    sections = random_forcing.astype(jnp.float32).reshape(N_TM, BLOCK_TICKS, CHANNELS)

    def convolve(section):
        padded = jnp.concatenate([section, jnp.zeros_like(section)], axis=0)
        spectra = jnp.fft.fft(padded, axis=0)
        return jnp.real(jnp.fft.ifft(spectra * eigen_root_table, axis=0)).astype(jnp.float32)
    last_trailing = convolve(sections[N_TM - 1])[BLOCK_TICKS:]

    def conv_step(trailing, section):
        entire = convolve(section)
        return (entire[BLOCK_TICKS:], entire[:BLOCK_TICKS] + trailing)
    unused, noise_sequence = lax.scan(conv_step, last_trailing, sections)
    forcing_kicks = sudden_shrink.reshape(N_TM, BLOCK_TICKS)

    def local_scan(paired):
        section, factors = paired
        tick_log_growth = jnp.log(factors)[:, None] - lane_fading_speed[None, :]
        power_entries = (factors * factors)[:, None]
        weights = jnp.sqrt(1.0 - power_entries + power_entries * (-jnp.expm1(-2.0 * lane_fading_speed))[None, :])
        return lax.associative_scan(combine, (tick_log_growth, weights * section), axis=0)

    def section_sums(paired):
        logs, states = local_scan(paired)
        return (logs[-1], states[-1])
    section_logarithm_sum, section_final_state = lax.map(section_sums, (noise_sequence, forcing_kicks))

    def prefix(carried, item):
        return (combine(carried, item), carried)
    zeroes = jnp.zeros((CHANNELS,), jnp.float32)
    entire_total, preceding_input = lax.scan(prefix, (zeroes, zeroes), (section_logarithm_sum, section_final_state))
    opening = entire_total[1] / -jnp.expm1(entire_total[0])

    def section_output(packed):
        paired, before_log, before_state = packed
        logs, states = local_scan(paired)
        incoming = jnp.exp(before_log) * opening + before_state
        return states + jnp.exp(logs) * incoming[None, :]
    field_output = lax.map(section_output, ((noise_sequence, forcing_kicks), preceding_input[0], preceding_input[1]))
    return field_output.reshape(TIME, CHANNELS)
```

```python
import functools

import jax
import jax.numpy as jnp
import ml_dtypes
import numpy as np
from jax import lax
from jax.experimental import pallas as pl
from jax.experimental.pallas import tpu as pltpu
from jax.sharding import PartitionSpec as P

MESH = pl.DeviceIdType.MESH
F32 = jnp.float32
BF16 = jnp.bfloat16
MEMBERS = 16


def split(table):
    high = table.astype(ml_dtypes.bfloat16)
    low = (table - high.astype(np.float64)).astype(ml_dtypes.bfloat16)
    return high, low


@functools.lru_cache
def tables(length):
    half = length // 2
    t = np.arange(length)
    even = 2 * np.arange(half)
    odd = even + 1

    def basis(f, function):
        return function(2.0 * np.pi * (np.outer(f, t) % (2 * length)) / (2 * length))

    even_sine = basis(even, np.sin)
    even_sine[0] = np.cos(np.pi * t)
    rows = np.concatenate([basis(even, np.cos), even_sine, basis(odd, np.cos), basis(odd, np.sin)])
    forward = np.concatenate(split(rows), axis=1)
    runs = length // 8
    order = (np.arange(8)[None, :] * runs + np.arange(runs)[:, None]).reshape(-1)
    high, low = split(rows.T[order])
    parts = []
    for k in range(2):
        at = slice(k * length, (k + 1) * length)
        parts += [high[:, at], high[:, at], low[:, at]]
    return forward, np.concatenate(parts, axis=1)


def flipped(tile):
    at = 7 - lax.broadcasted_iota(jnp.int32, tile.shape, 0)
    return jnp.take_along_axis(tile, at, axis=0)


def fold(e_ref, es_ref, lane, length):
    half = length // 2
    scale = 1.0 / (2 * length)
    row = lax.broadcasted_iota(jnp.int32, (8, 128), 0)
    for b in range(half // 8):
        value = e_ref[lane, pl.ds(16 * b, 8, stride=2), :]
        if b:
            mirror = flipped(e_ref[lane, pl.ds(2 * length - 14 - 16 * b, 8, stride=2), :])
        else:
            mirror = flipped(e_ref[lane, pl.ds(2 * length - 16, 8, stride=2), :])
            mirror = jnp.where(row == 0, 0.0, pltpu.roll(mirror, 1, 0))
        total = (value + mirror) * scale
        es_ref[lane, 8 * b : 8 * b + 8, :] = total
        if b == 0:
            middle = jnp.broadcast_to(e_ref[lane, length : length + 1, :], (8, 128)) * scale
            total = jnp.where(row == 0, middle, total)
        es_ref[lane, half + 8 * b : half + 8 * b + 8, :] = total
        value = e_ref[lane, pl.ds(16 * b + 1, 8, stride=2), :]
        mirror = flipped(e_ref[lane, pl.ds(2 * length - 15 - 16 * b, 8, stride=2), :])
        es_ref[lane, 2 * half + 8 * b : 2 * half + 8 * b + 8, :] = (value + mirror) * scale


def over_runs(state, decay):
    row = lax.broadcasted_iota(jnp.int32, state.shape, 0)
    for step in (1, 2, 4):
        reach = row >= step
        state = jnp.where(reach, decay * pltpu.roll(state, step, 0) + state, state)
        decay = jnp.where(reach, decay * pltpu.roll(decay, step, 0), decay)
    return state, decay


def weight(burst, spread):
    power = burst * burst
    return jnp.sqrt((1.0 - power) + power * spread)


def fields(
    length, sections, v_hbm, e_hbm, forward_hbm, inverse_hbm, rows_ref, rate_ref, burst_ref, logs_ref,
    x_ref, carry_ref, reach_ref, grown_ref, incoming_ref,
    v_ref, e_ref, forward_ref, inverse_ref, es_ref, earlier_ref, twice_ref, value_ref, scaled_ref, p_ref, q_ref, lead_ref,
    own_ref, next_ref, next_burst_ref, ends_ref, a_ref, c_ref, c_in_ref, half_ref, pair_ref, chips_ref, groups_ref,
    member_logs_ref, group_logs_ref, group_log_ref, chip_out_ref, group_out_ref, give_ref, take_ref,
    v_sem, e_sem, t_sem, noise_send, noise_recv, burst_sem, c_sem, pair_sem, give_sem,
    logs_send, logs_recv, chips_send, chips_recv, groups_send, groups_recv, glogs_send, glogs_recv,
):
    width = v_hbm.shape[1]
    chunk = 256
    chunks = width // chunk
    lanes = width // 128
    half = length // 2
    runs = length // 8
    groups = sections // MEMBERS
    chips = MEMBERS // 2
    me = lax.axis_index("tm")
    group, member = me // MEMBERS, me % MEMBERS
    chip, core = member // 2, member % 2
    after, before = (me + 1) % sections, (me + sections - 1) % sections
    partner = group * MEMBERS + chip * 2 + (1 - core)

    def remote(source, target, send, recv, device):
        return pltpu.make_async_remote_copy(
            src_ref=source, dst_ref=target, send_sem=send, recv_sem=recv, device_id={"tm": device}, device_id_type=MESH
        )

    def columns(i):
        return pl.ds(pl.multiple_of(i * chunk, chunk), chunk)

    members = [group * MEMBERS + (member + k) % MEMBERS for k in range(1, MEMBERS)]
    chip_peers = [group * MEMBERS + ((chip + k) % chips) * 2 + core for k in range(1, chips)]
    group_peers = [((group + k) % groups) * MEMBERS + member for k in range(1, groups)]

    barrier = pltpu.get_barrier_semaphore()
    for device in [after, before] + members + group_peers:
        pl.semaphore_signal(barrier, inc=1, device_id={"tm": device}, device_id_type=MESH)

    local = [
        pltpu.make_async_copy(v_hbm, v_ref.at[pl.ds(0, length)], v_sem.at[0]),
        pltpu.make_async_copy(v_hbm, v_ref.at[pl.ds(length, length)], v_sem.at[1]),
        pltpu.make_async_copy(forward_hbm, forward_ref, t_sem.at[0]),
        pltpu.make_async_copy(inverse_hbm, inverse_ref, t_sem.at[1]),
    ]

    def table(lane):
        return pltpu.make_async_copy(e_hbm.at[:, pl.ds(pl.multiple_of(lane * 128, 128), 128)], e_ref.at[lane], e_sem.at[lane])

    for lane in range(lanes):
        table(lane).start()
    for copy in local:
        copy.start()

    product = jnp.ones((8, 128), F32)
    for j in range(runs):
        column = jnp.broadcast_to(burst_ref[:, j : j + 1], (8, 128))
        own_ref[8 * j : 8 * j + 8, :] = column
        product = product * column
        grown_ref[8 * j : 8 * j + 8, :] = product
    ends_ref[0] = product

    pl.semaphore_wait(barrier, 2 + (MEMBERS - 1) + (groups - 1))

    burst_copy = remote(burst_ref, next_burst_ref, burst_sem.at[0], burst_sem.at[1], before)
    burst_copy.start()
    logs_copies = [
        remote(logs_ref, member_logs_ref.at[member], logs_send.at[k], logs_recv.at[k], device)
        for k, device in enumerate(members)
    ]
    for copy in logs_copies:
        copy.start()

    def noise(i):
        return remote(v_hbm.at[:, columns(i)], earlier_ref.at[:, columns(i)], noise_send.at[i], noise_recv.at[i], after)

    noise(0).start()
    noise(1).start()

    def fold_step(lane, carry):
        table(lane).wait()
        fold(e_ref, es_ref, lane, length)
        return carry

    lax.fori_loop(0, lanes, fold_step, 0)

    for copy in local:
        copy.wait()
    burst_copy.wait()
    product = jnp.ones((8, 128), F32)
    for j in range(runs):
        column = jnp.broadcast_to(next_burst_ref[:, j : j + 1], (8, 128))
        next_ref[8 * j : 8 * j + 8, :] = column
        product = product * column
    ends_ref[1] = product

    def transform(i, data, sign):
        value_ref[...] = jnp.dot(forward_ref[...], data, preferred_element_type=F32)
        for part in range(4):
            at = (0, half, 2 * half, 2 * half)[part]
            base = 3 * length * (part // 2) + half * (part % 2)
            for side in range(2):
                cut = slice(128 * side, 128 * side + 128)
                scaled = value_ref[half * part : half * part + half, cut] * es_ref[2 * i + side, at : at + half, :]
                if part >= 2 and sign < 0:
                    scaled = -scaled
                high = scaled.astype(BF16)
                low = (scaled - high.astype(F32)).astype(BF16)
                scaled_ref[base : base + half, cut] = high
                scaled_ref[base + length : base + length + half, cut] = low
                scaled_ref[base + 2 * length : base + 2 * length + half, cut] = high

    def row_of(index, lane_columns):
        return jnp.broadcast_to(rows_ref[index : index + 1, lane_columns], (8, 128))

    def early(i, carry):
        transform(i, v_ref[:, columns(i)], 1)
        cut = 3 * length
        p_ref[...] = jnp.dot(inverse_ref[:, :cut], scaled_ref[:cut, :], preferred_element_type=F32)
        q_ref[...] = jnp.dot(inverse_ref[:, cut:], scaled_ref[cut:, :], preferred_element_type=F32)
        for side in range(2):
            lane = 2 * i + side
            cols = pl.ds(pl.multiple_of(lane * 128, 128), 128)
            keep, keep_run, spread = row_of(0, cols), row_of(1, cols), row_of(2, cols)
            here = jnp.zeros((8, 128), F32)
            there = jnp.zeros((8, 128), F32)
            for j in range(runs):
                at = slice(8 * j, 8 * j + 8)
                p = p_ref[at, 128 * side : 128 * side + 128]
                q = q_ref[at, 128 * side : 128 * side + 128]
                lead = p + q
                lead_ref[lane, at, :] = lead
                burst = own_ref[at, :]
                here = (burst * keep) * here + weight(burst, spread) * lead
                burst = next_ref[at, :]
                there = (burst * keep) * there + weight(burst, spread) * (p - q)
            here, _ = over_runs(here, ends_ref[0] * keep_run)
            there, _ = over_runs(there, ends_ref[1] * keep_run)
            a_ref[pl.ds(lane, 1), :] = here[7:8, :]
            c_ref[pl.ds(lane, 1), :] = there[7:8, :]

        @pl.when((i % 2 == 1) & (i < chunks - 1))
        def _():
            noise(2 + i // 2).start()

        return carry

    lax.fori_loop(0, chunks, early, 0)

    c_copy = remote(c_ref, c_in_ref, c_sem.at[0], c_sem.at[1], after)
    c_copy.start()
    sent_early = 2 + (chunks - 1) // 2

    for copy in logs_copies:
        copy.wait()
    member_logs_ref[pl.ds(member, 1)] = logs_ref[...].reshape(1, 1, 128)
    logs_of = [jnp.broadcast_to(member_logs_ref[k], (8, 128)) for k in range(MEMBERS)]
    whole = sum(logs_of[1:], logs_of[0])
    group_log_ref[...] = whole[0:1, :]
    group_logs_ref[pl.ds(group, 1)] = whole[0:1, :].reshape(1, 1, 128)
    glogs_copies = [
        remote(group_log_ref, group_logs_ref.at[group], glogs_send.at[k], glogs_recv.at[k], device)
        for k, device in enumerate(group_peers)
    ]
    for copy in glogs_copies:
        copy.start()

    own_half = pl.ds(pl.multiple_of(core * 8, 8), 8)
    other_half = pl.ds(pl.multiple_of((1 - core) * 8, 8), 8)
    pair_copy = remote(half_ref.at[0], pair_ref, pair_sem.at[0], pair_sem.at[1], partner)
    chip_copies = [
        remote(chip_out_ref, chips_ref.at[chip], chips_send.at[k], chips_recv.at[k], device)
        for k, device in enumerate(chip_peers)
    ]
    group_copies = [
        remote(group_out_ref, groups_ref.at[group], groups_send.at[k], groups_recv.at[k], device)
        for k, device in enumerate(group_peers)
    ]
    give_copy = remote(give_ref, take_ref, give_sem.at[0], give_sem.at[1], partner)

    def log_of(index):
        return jnp.broadcast_to(member_logs_ref[index], (8, 128))

    def pair_states():
        mine, theirs = half_ref[1], pair_ref[...]
        first = jnp.where(core == 0, mine, theirs)
        second = jnp.where(core == 0, theirs, mine)
        return first, second

    def exchange_pair():
        c_copy.wait()
        half_ref[0] = a_ref[other_half, :] + c_in_ref[other_half, :]
        half_ref[1] = a_ref[own_half, :] + c_in_ref[own_half, :]
        pair_copy.start()

    def exchange_chips():
        pair_copy.wait()
        first, second = pair_states()
        rate = rate_ref[own_half, :]
        total = jnp.exp(log_of(2 * chip + 1)[0:8] - length * rate) * first + second
        chip_out_ref[...] = total
        chips_ref[pl.ds(chip, 1)] = total.reshape(1, 8, 128)
        for copy in chip_copies:
            copy.start()

    def exchange_groups():
        for copy in chip_copies:
            copy.wait()
        rate = rate_ref[own_half, :]
        state = jnp.zeros((8, 128), F32)
        log = jnp.zeros((8, 128), F32)
        before_state, before_log = state, log
        for k in range(chips):
            here = chip == k
            before_state = jnp.where(here, state, before_state)
            before_log = jnp.where(here, log, before_log)
            step = (log_of(2 * k) + log_of(2 * k + 1)) - (2 * length) * rate
            state = jnp.exp(step) * state + chips_ref[k]
            log = log + step
        half_ref[2] = before_state
        half_ref[3] = before_log
        group_out_ref[...] = state
        groups_ref[pl.ds(group, 1)] = state.reshape(1, 8, 128)
        for copy in group_copies:
            copy.start()

    def exchange_back():
        for copy in group_copies:
            copy.wait()
        for copy in glogs_copies:
            copy.wait()
        rate = rate_ref[own_half, :]
        state = jnp.zeros((8, 128), F32)
        log = jnp.zeros((8, 128), F32)
        for k in range(groups):
            at = (group + k) % groups
            step = jnp.broadcast_to(group_logs_ref[at], (8, 128)) - (MEMBERS * length) * rate
            state = jnp.exp(step) * state + groups_ref[at]
            log = log + step
        opening = state / (1.0 - jnp.exp(log))
        first_in = jnp.exp(half_ref[3]) * opening + half_ref[2]
        first, _ = pair_states()
        second_in = jnp.exp(log_of(2 * chip) - length * rate) * first_in + first
        incoming_ref[own_half, :] = jnp.where(core == 0, first_in, second_in)
        give_ref[...] = jnp.where(core == 0, second_in, first_in)
        give_copy.start()

    def late(i, carry):
        @pl.when(i + sent_early < chunks)
        def _():
            noise(i + sent_early).start()

        noise(i).wait_recv()
        block = earlier_ref[:, columns(i)]
        twice_ref[0:length, :] = block
        twice_ref[length : 2 * length, :] = block
        transform(i, twice_ref[...], -1)
        p_ref[...] = jnp.dot(inverse_ref[...], scaled_ref[...], preferred_element_type=F32)
        for side in range(2):
            lane = 2 * i + side
            cols = pl.ds(pl.multiple_of(lane * 128, 128), 128)
            keep, keep_run, spread = row_of(0, cols), row_of(1, cols), row_of(2, cols)
            state = jnp.zeros((8, 128), F32)
            for j in range(runs):
                at = slice(8 * j, 8 * j + 8)
                burst = own_ref[at, :]
                series = lead_ref[lane, at, :] + p_ref[at, 128 * side : 128 * side + 128]
                state = (burst * keep) * state + weight(burst, spread) * series
                x_ref[lane, at, :] = state
            state, decay = over_runs(state, ends_ref[0] * keep_run)
            row = lax.broadcasted_iota(jnp.int32, (8, 128), 0)
            carry_ref[lane] = jnp.where(row == 0, 0.0, pltpu.roll(state, 1, 0))
            reach_ref[lane] = jnp.where(row == 0, 1.0, pltpu.roll(decay, 1, 0))
        for at, step in ((1, exchange_pair), (2, exchange_chips), (4, exchange_groups), (6, exchange_back)):
            pl.when(i == at)(step)
        return carry

    lax.fori_loop(0, chunks, late, 0)
    give_copy.wait()
    incoming_ref[other_half, :] = take_ref[...]

    def drain(i, carry):
        noise(i).wait_send()
        return carry

    lax.fori_loop(0, chunks, drain, 0)


def close(length, x_ref, carry_ref, reach_ref, grown_ref, incoming_ref, rows_ref, out_hbm, stage_ref, sem):
    lanes = x_ref.shape[0]
    runs = length // 8

    def out(lane):
        return pltpu.make_async_copy(
            stage_ref.at[lane], out_hbm.at[:, pl.ds(pl.multiple_of(lane * 128, 128), 128)], sem.at[lane]
        )

    def step(lane, carry):
        cols = pl.ds(pl.multiple_of(lane * 128, 128), 128)
        keep = jnp.broadcast_to(rows_ref[0:1, cols], (8, 128))
        incoming = jnp.broadcast_to(incoming_ref[pl.ds(lane, 1), :], (8, 128))
        state = (carry_ref[lane] + reach_ref[lane] * incoming) * keep
        for j in range(runs):
            at = slice(8 * j, 8 * j + 8)
            stage_ref[lane, pl.ds(j, 8, stride=runs), :] = x_ref[lane, at, :] + grown_ref[at, :] * state
            state = state * keep
        out(lane).start()
        return carry

    lax.fori_loop(0, lanes, step, 0)

    def drain(lane, carry):
        out(lane).wait()
        return carry

    lax.fori_loop(0, lanes, drain, 0)


def shards(sections, random_forcing, eigen_root_table, lane_fading_speed, sudden_shrink):
    length, width = random_forcing.shape
    lanes, runs, half = width // 128, length // 8, length // 2
    chunk = 256
    chunks = width // chunk
    groups, chips = sections // MEMBERS, MEMBERS // 2
    forward, inverse = tables(length)
    rate = lane_fading_speed
    rows = jnp.stack([jnp.exp(-rate), jnp.exp(-runs * rate), -jnp.expm1(-2.0 * rate)])
    rows = jnp.pad(rows, ((0, 5), (0, 0)))
    burst = jnp.pad(sudden_shrink.reshape(8, runs), ((0, 0), (0, 128 - runs)))
    logs = jnp.broadcast_to(jnp.sum(jnp.log(sudden_shrink)), (1, 128))
    anywhere = pl.BlockSpec(memory_space=pl.ANY)
    vmem = pl.BlockSpec(memory_space=pltpu.VMEM)
    dma = pltpu.SemaphoreType.DMA
    tile = pltpu.VMEM((8, 128), F32)
    results = pl.pallas_call(
        functools.partial(fields, length, sections),
        name="fields",
        out_shape=[
            jax.ShapeDtypeStruct((lanes, length, 128), F32),
            jax.ShapeDtypeStruct((lanes, 8, 128), F32),
            jax.ShapeDtypeStruct((lanes, 8, 128), F32),
            jax.ShapeDtypeStruct((length, 128), F32),
            jax.ShapeDtypeStruct((lanes, 128), F32),
        ],
        in_specs=[anywhere] * 4 + [vmem] * 4,
        out_specs=[vmem] * 5,
        scratch_shapes=[
            pltpu.VMEM((2 * length, width), BF16),
            pltpu.VMEM((lanes, 2 * length, 128), F32),
            pltpu.VMEM((2 * length, 2 * length), BF16),
            pltpu.VMEM((length, 6 * length), BF16),
            pltpu.VMEM((lanes, 3 * half, 128), F32),
            pltpu.VMEM((length, width), BF16),
            pltpu.VMEM((2 * length, chunk), BF16),
            pltpu.VMEM((2 * length, chunk), F32),
            pltpu.VMEM((6 * length, chunk), BF16),
            pltpu.VMEM((length, chunk), F32),
            pltpu.VMEM((length, chunk), F32),
            pltpu.VMEM((lanes, length, 128), F32),
            pltpu.VMEM((length, 128), F32),
            pltpu.VMEM((length, 128), F32),
            tile,
            pltpu.VMEM((2, 8, 128), F32),
            pltpu.VMEM((lanes, 128), F32),
            pltpu.VMEM((lanes, 128), F32),
            pltpu.VMEM((lanes, 128), F32),
            pltpu.VMEM((4, 8, 128), F32),
            tile,
            pltpu.VMEM((chips, 8, 128), F32),
            pltpu.VMEM((groups, 8, 128), F32),
            pltpu.VMEM((MEMBERS, 1, 128), F32),
            pltpu.VMEM((groups, 1, 128), F32),
            pltpu.VMEM((1, 128), F32),
            tile,
            tile,
            tile,
            tile,
            dma((2,)),
            dma((lanes,)),
            dma((2,)),
            dma((chunks,)),
            dma((chunks,)),
            dma((2,)),
            dma((2,)),
            dma((2,)),
            dma((2,)),
            dma((MEMBERS - 1,)),
            dma((MEMBERS - 1,)),
            dma((chips - 1,)),
            dma((chips - 1,)),
            dma((groups - 1,)),
            dma((groups - 1,)),
            dma((groups - 1,)),
            dma((groups - 1,)),
        ],
        compiler_params=pltpu.CompilerParams(
            collective_id=0, has_side_effects=True, vmem_limit_bytes=48 * 2**20
        ),
    )(random_forcing, eigen_root_table, jnp.asarray(forward), jnp.asarray(inverse), rows, rate.reshape(lanes, 128), burst, logs)
    return pl.pallas_call(
        functools.partial(close, length),
        name="close",
        out_shape=jax.ShapeDtypeStruct((length, width), F32),
        in_specs=[vmem] * 6,
        out_specs=anywhere,
        scratch_shapes=[pltpu.VMEM((lanes, length, 128), F32), dma((lanes,))],
    )(*results, rows)


def solution(mesh):
    return jax.shard_map(
        functools.partial(shards, mesh.shape["tm"]),
        mesh=mesh,
        in_specs=(P("tm", "chan"), P(None, "chan"), P("chan"), P("tm")),
        out_specs=P("tm", "chan"),
        check_vma=False,
    )
```

```python
import functools

import jax
import jax.numpy as jnp
import ml_dtypes
import numpy as np
from jax import lax
from jax.experimental import pallas as pl
from jax.experimental.pallas import tpu as pltpu
from jax.sharding import PartitionSpec as P

MESH = pl.DeviceIdType.MESH
F32 = jnp.float32
BF16 = jnp.bfloat16
MEMBERS = 16


def split(table):
    high = table.astype(ml_dtypes.bfloat16)
    low = (table - high.astype(np.float64)).astype(ml_dtypes.bfloat16)
    return high, low


@functools.lru_cache
def tables(length):
    half = length // 2
    t = np.arange(length)
    even = 2 * np.arange(half)
    odd = even + 1

    def basis(f, function):
        return function(2.0 * np.pi * (np.outer(f, t) % (2 * length)) / (2 * length))

    even_sine = basis(even, np.sin)
    even_sine[0] = np.cos(np.pi * t)
    rows = np.concatenate([basis(even, np.cos), even_sine, basis(odd, np.cos), basis(odd, np.sin)])
    forward = np.concatenate(split(rows), axis=1)
    runs = length // 8
    order = (np.arange(8)[None, :] * runs + np.arange(runs)[:, None]).reshape(-1)
    high, low = split(rows.T[order])
    parts = []
    for k in range(2):
        at = slice(k * length, (k + 1) * length)
        parts += [high[:, at], low[:, at]]
    return forward, np.concatenate(parts, axis=1)


def flipped(tile):
    at = 7 - lax.broadcasted_iota(jnp.int32, tile.shape, 0)
    return jnp.take_along_axis(tile, at, axis=0)


def fold(e_ref, es_ref, lane, length):
    half = length // 2
    scale = 1.0 / (2 * length)
    row = lax.broadcasted_iota(jnp.int32, (8, 128), 0)
    for b in range(half // 8):
        value = e_ref[lane, pl.ds(16 * b, 8, stride=2), :]
        if b:
            mirror = flipped(e_ref[lane, pl.ds(2 * length - 14 - 16 * b, 8, stride=2), :])
        else:
            mirror = flipped(e_ref[lane, pl.ds(2 * length - 16, 8, stride=2), :])
            mirror = jnp.where(row == 0, 0.0, pltpu.roll(mirror, 1, 0))
        total = (value + mirror) * scale
        es_ref[lane, 8 * b : 8 * b + 8, :] = total
        if b == 0:
            middle = jnp.broadcast_to(e_ref[lane, length : length + 1, :], (8, 128)) * scale
            total = jnp.where(row == 0, middle, total)
        es_ref[lane, half + 8 * b : half + 8 * b + 8, :] = total
        value = e_ref[lane, pl.ds(16 * b + 1, 8, stride=2), :]
        mirror = flipped(e_ref[lane, pl.ds(2 * length - 15 - 16 * b, 8, stride=2), :])
        es_ref[lane, 2 * half + 8 * b : 2 * half + 8 * b + 8, :] = (value + mirror) * -scale


def over_runs(state, decay):
    row = lax.broadcasted_iota(jnp.int32, state.shape, 0)
    for step in (1, 2, 4):
        reach = row >= step
        state = jnp.where(reach, decay * pltpu.roll(state, step, 0) + state, state)
        decay = jnp.where(reach, decay * pltpu.roll(decay, step, 0), decay)
    return state, decay


def weighted(value, loss, power, spread):
    square = loss + power * spread
    return square * lax.rsqrt(square) * value


def spread_of(rate):
    x = 2.0 * rate
    series = 1.0 - x * (1.0 / 6.0)
    for k in (5, 4, 3, 2):
        series = 1.0 - x * (1.0 / k) * series
    return x * series


def fields(
    length, sections, v_hbm, e_hbm, forward_hbm, inverse_hbm, rate_hbm, burst_hbm, x_ref,
    v_ref, e_ref, forward_ref, inverse_ref, rate_ref, burst_line, es_ref, earlier_ref, twice_ref,
    value0_ref, value1_ref, scaled0_ref, scaled1_ref, p0_ref, p1_ref, q0_ref, q1_ref, lead_ref,
    own_ref, next_ref, burst_ref, next_burst_ref, ends_ref, carry_ref, reach_ref, incoming_ref, logs_ref,
    a_ref, c_ref, pair_out_ref, pair_in_ref, before_ref, chips_ref, groups_ref,
    member_logs_ref, group_logs_ref, group_log_ref, chip_out_ref, group_out_ref, give_ref, take_ref,
    t_sem, e_sem, noise_send, noise_recv, burst_sem, pair_sem, give_sem, logs_sem, chips_sem, groups_sem, glogs_sem,
):
    width = v_hbm.shape[1]
    chunk = 256
    chunks = width // chunk
    lanes = width // 128
    half = length // 2
    runs = length // 8
    groups = sections // MEMBERS
    chips = MEMBERS // 2
    me = lax.axis_index("tm")
    group, member = me // MEMBERS, me % MEMBERS
    chip, core = member // 2, member % 2
    after, before = (me + 1) % sections, (me + sections - 1) % sections
    partner = group * MEMBERS + chip * 2 + (1 - core)
    values, scaleds = (value0_ref, value1_ref), (scaled0_ref, scaled1_ref)
    ps, qs = (p0_ref, p1_ref), (q0_ref, q1_ref)

    def remote(source, target, send, recv, device):
        return pltpu.make_async_remote_copy(
            src_ref=source, dst_ref=target, send_sem=send, recv_sem=recv, device_id={"tm": device}, device_id_type=MESH
        )

    def columns(i):
        return pl.ds(pl.multiple_of(i * chunk, chunk), chunk)

    members = [group * MEMBERS + (member + k) % MEMBERS for k in range(1, MEMBERS)]
    chip_peers = [group * MEMBERS + ((chip + k) % chips) * 2 + core for k in range(1, chips)]
    group_peers = [((group + k) % groups) * MEMBERS + member for k in range(1, groups)]

    barrier = pltpu.get_barrier_semaphore()
    for device in [after, before] + group_peers + members:
        pl.semaphore_signal(barrier, inc=1, device_id={"tm": device}, device_id_type=MESH)

    def arrived(ref, sem):
        pltpu.make_async_copy(ref, ref, sem).wait()

    for lane in range(lanes):
        pltpu.make_async_copy(e_hbm.at[:, pl.ds(lane * 128, 128)], e_ref.at[lane], e_sem.at[lane // 4]).start()
    pltpu.make_async_copy(burst_hbm, burst_line, t_sem.at[0]).start()
    for k in range(2):
        pltpu.make_async_copy(v_hbm, v_ref.at[pl.ds(k * length, length)], t_sem.at[1]).start()
    pltpu.make_async_copy(forward_hbm, forward_ref, t_sem.at[2]).start()
    for k, source in enumerate((0, 0, 1, 2, 2, 3)):
        pltpu.make_async_copy(
            inverse_hbm.at[:, pl.ds(source * length, length)], inverse_ref.at[:, pl.ds(k * length, length)], t_sem.at[3]
        ).start()
    pltpu.make_async_copy(rate_hbm, rate_ref, t_sem.at[4]).start()

    def broadcasts(source_ref, target_ref):
        product = jnp.ones((8, 128), F32)
        for j in range(runs):
            column = jnp.broadcast_to(source_ref[:, j : j + 1], (8, 128))
            at = slice(8 * j, 8 * j + 8)
            power = column * column
            target_ref[0, at, :] = column
            target_ref[1, at, :] = 1.0 - power
            target_ref[2, at, :] = power
            product = product * column
            if source_ref is burst_ref:
                x_ref[lanes, 8 * j : 8 * j + 8, :] = product
        return product

    def noise(i):
        return remote(v_hbm.at[:, columns(i)], earlier_ref.at[:, columns(i)], noise_send.at[0], noise_recv.at[i], after)

    burst_copy = remote(burst_ref, next_burst_ref, burst_sem.at[0], burst_sem.at[1], before)

    def fold_step(lane, carry):
        @pl.when(lane % 4 == 0)
        def _():
            four = e_ref.at[pl.ds(pl.multiple_of(lane, 4), 4)]
            arrived(four, e_sem.at[lane // 4])

        fold(e_ref, es_ref, lane, length)
        return carry

    lax.fori_loop(0, lanes // 2, fold_step, 0)
    arrived(burst_line, t_sem.at[0])
    line = jnp.concatenate([burst_line[k : k + 1, :] for k in range(length // 128)], axis=1)
    burst_ref[:, 0:runs] = jnp.concatenate([line[:, runs * k : runs * k + runs] for k in range(8)], axis=0)
    burst_ref[:, runs:128] = jnp.ones((8, 128 - runs), F32)
    logs_ref[...] = jnp.broadcast_to(jnp.sum(jnp.log(line), axis=1, keepdims=True), (1, 128))

    pl.semaphore_wait(barrier, 2 + (MEMBERS - 1) + (groups - 1))
    burst_copy.start()
    noise(0).start()
    noise(1).start()
    for device in members:
        remote(logs_ref, member_logs_ref.at[member], logs_sem.at[0], logs_sem.at[1], device).start()

    ends_ref[0] = broadcasts(burst_ref, own_ref)
    lax.fori_loop(lanes // 2, lanes, fold_step, 0)
    for k, ref in ((4, rate_ref), (1, v_ref), (2, forward_ref), (3, inverse_ref)):
        arrived(ref, t_sem.at[k])
    x_ref[lanes + 1, 0:lanes, :] = rate_ref[...]

    def rate_rows(lane):
        rate = jnp.broadcast_to(rate_ref[pl.ds(lane, 1), :], (8, 128))
        return jnp.exp(-rate), jnp.exp(-runs * rate), spread_of(rate)

    def forward(data, slot, part):
        at = slice(half * part, half * part + half)
        values[slot][at, :] = jnp.dot(forward_ref[at, :], data, preferred_element_type=F32)

    def scale(i, slot, part):
        at = (0, half, 2 * half, 2 * half)[part]
        base = 3 * length * (part // 2) + half * (part % 2)
        for side in range(2):
            cut = slice(128 * side, 128 * side + 128)
            scaled = values[slot][half * part : half * part + half, cut] * es_ref[2 * i + side, at : at + half, :]
            high = scaled.astype(BF16)
            low = (scaled - high.astype(F32)).astype(BF16)
            scaleds[slot][base : base + half, cut] = high
            scaleds[slot][base + length : base + length + half, cut] = low
            scaleds[slot][base + 2 * length : base + 2 * length + half, cut] = high

    def early_inverse(slot, part):
        target, cut = (ps, qs)[part // 2], slice(3 * length * (part // 2), 3 * length * (part // 2) + 3 * length)
        at = slice(half * (part % 2), half * (part % 2) + half)
        target[slot][at, :] = jnp.dot(inverse_ref[at, cut], scaleds[slot][cut, :], preferred_element_type=F32)

    def early_scan(i, slot, states, piece, pieces):
        for side in range(2):
            lane = 2 * i + side
            if piece == 0:
                states[side] = rate_rows(lane) + (jnp.zeros((8, 128), F32), jnp.zeros((8, 128), F32))
            keep, keep_run, spread, here, there = states[side]
            for j in range(runs * piece // pieces, runs * (piece + 1) // pieces):
                at = slice(8 * j, 8 * j + 8)
                p = ps[slot][at, 128 * side : 128 * side + 128]
                q = qs[slot][at, 128 * side : 128 * side + 128]
                lead = p - q
                lead_ref[lane, at, :] = lead
                force = weighted(lead, own_ref[1, at, :], own_ref[2, at, :], spread)
                here = (own_ref[0, at, :] * keep) * here + force
                force = weighted(p + q, next_ref[1, at, :], next_ref[2, at, :], spread)
                there = (next_ref[0, at, :] * keep) * there + force
            states[side] = (keep, keep_run, spread, here, there)
            if piece < pieces - 1:
                continue
            here, _ = over_runs(here, ends_ref[0] * keep_run)
            there, _ = over_runs(there, ends_ref[1] * keep_run)
            a_ref[pl.ds(lane, 1), :] = here[7:8, :]
            c_ref[pl.ds(lane, 1), :] = there[7:8, :]

    def whole(scan, i, slot):
        scan(i, slot, [None, None], 0, 1)

    def step(i, slot, data, inverse, scan):
        states = [None, None]
        for part in range(4):
            forward(data, 1 - slot, part)
            scan((i + chunks - 1) % chunks, 1 - slot, states, part, 8)
        for part in range(4):
            inverse(slot, part)
            scale(i + 1, 1 - slot, part)
            scan((i + chunks - 1) % chunks, 1 - slot, states, part + 4, 8)

    def early_step(i, slot):
        step(i, slot, v_ref[:, columns(i + 1)], early_inverse, early_scan)

    for part in range(4):
        forward(v_ref[:, columns(0)], 0, part)
        scale(0, 0, part)
    def early_pair(u, carry):
        noise(2 + u).start()
        early_step(2 * u, 0)

        @pl.when(u == 0)
        def _():
            burst_copy.wait()
            ends_ref[1] = broadcasts(next_burst_ref, next_ref)

        early_step(2 * u + 1, 1)
        return carry

    lax.fori_loop(0, chunks // 2 - 1, early_pair, 0)
    noise(chunks // 2 + 1).start()
    early_step(chunks - 2, 0)
    states = [None, None]
    for part in range(4):
        early_inverse(1, part)
        early_scan(chunks - 2, 0, states, part, 4)
    whole(early_scan, chunks - 1, 1)
    sent_early = chunks // 2 + 2

    own_half = pl.ds(pl.multiple_of(core * 8, 8), 8)
    other_half = pl.ds(pl.multiple_of((1 - core) * 8, 8), 8)
    pair_copy = remote(pair_out_ref, pair_in_ref, pair_sem.at[0], pair_sem.at[1], partner)
    give_copy = remote(give_ref, take_ref, give_sem.at[0], give_sem.at[1], partner)
    pair_out_ref[0] = a_ref[other_half, :]
    pair_out_ref[1] = c_ref[other_half, :]
    pair_copy.start()

    for k in range(2):
        arrived(member_logs_ref.at[pl.ds(0, MEMBERS - 1)], logs_sem.at[k])
    member_logs_ref[pl.ds(member, 1)] = logs_ref[...].reshape(1, 1, 128)
    logs_of = [member_logs_ref[k] for k in range(MEMBERS)]
    group_log_ref[0:1, :] = sum(logs_of[1:], logs_of[0])
    group_log_ref[1:2, :] = logs_of[0]
    group_logs_ref[pl.ds(group, 1)] = group_log_ref[...].reshape(1, 2, 128)
    for device in group_peers:
        remote(group_log_ref, group_logs_ref.at[group], glogs_sem.at[0], glogs_sem.at[1], device).start()

    def log_of(index):
        return jnp.broadcast_to(member_logs_ref[index], (8, 128)) - length * rate_ref[own_half, :]

    def of_first(k):
        own = (a_ref, c_ref)[k][own_half, :]
        return jnp.where(core == 0, own, pair_in_ref[k])

    def of_second(k):
        own = (a_ref, c_ref)[k][own_half, :]
        return jnp.where(core == 0, pair_in_ref[k], own)

    def exchange_chips():
        pair_copy.wait()
        chip_out_ref[0] = jnp.exp(log_of(2 * chip + 1)) * of_first(0) + of_first(1) + of_second(0)
        chip_out_ref[1] = of_second(1)
        for device in chip_peers:
            remote(chip_out_ref, chips_ref.at[chip], chips_sem.at[0], chips_sem.at[1], device).start()
        chips_ref[pl.ds(chip, 1)] = chip_out_ref[...].reshape(1, 2, 8, 128)

    def exchange_groups():
        for k in range(2):
            arrived(chips_ref.at[pl.ds(0, chips - 1)], chips_sem.at[k])
        state = jnp.zeros((8, 128), F32)
        log, tail = state, state
        before = (state, log, tail)
        for k in range(chips):
            here = chip == k
            before = tuple(jnp.where(here, new, old) for new, old in zip((state, log, tail), before))
            second = log_of(2 * k + 1)
            step = log_of(2 * k) + second
            state = jnp.exp(step) * state + jnp.exp(second) * tail + chips_ref[k, 0]
            tail = chips_ref[k, 1]
            log = log + step
        group_out_ref[0] = state
        group_out_ref[1] = tail
        for device in group_peers:
            remote(group_out_ref, groups_ref.at[group], groups_sem.at[0], groups_sem.at[1], device).start()
        groups_ref[pl.ds(group, 1)] = group_out_ref[...].reshape(1, 2, 8, 128)
        for k in range(3):
            before_ref[k] = before[k]

    def exchange_back():
        for k in range(2):
            arrived(groups_ref.at[pl.ds(0, groups - 1)], groups_sem.at[k])
        for k in range(2):
            arrived(group_logs_ref.at[pl.ds(0, groups - 1)], glogs_sem.at[k])
        rate = rate_ref[own_half, :]
        entering = groups_ref[(group + groups - 1) % groups, 1]
        state = jnp.zeros((8, 128), F32)
        log, tail = state, entering
        for k in range(groups):
            at = (group + k) % groups
            total = jnp.broadcast_to(group_logs_ref[at, 0:1, :], (8, 128))
            first = jnp.broadcast_to(group_logs_ref[at, 1:2, :], (8, 128))
            step = total - (MEMBERS * length) * rate
            rest = (total - first) - ((MEMBERS - 1) * length) * rate
            state = jnp.exp(step) * state + jnp.exp(rest) * tail + groups_ref[at, 0]
            tail = groups_ref[at, 1]
            log = log + step
        opening = state / (1.0 - jnp.exp(log))
        log = before_ref[1]
        arriving = jnp.where(chip == 0, 0.0, jnp.exp(log - log_of(0)) * entering)
        first_in = jnp.exp(log) * opening + before_ref[0] + arriving
        tail = jnp.where(chip == 0, entering, before_ref[2])
        second_in = jnp.exp(log_of(2 * chip)) * first_in + of_first(0) + tail
        incoming_ref[own_half, :] = jnp.where(core == 0, first_in, second_in)
        give_ref[...] = jnp.where(core == 0, second_in, first_in)
        give_copy.start()

    def arrive(i):
        noise(i).wait_recv()

    def late_data(i):
        block = earlier_ref[:, columns(i)]
        twice_ref[0:length, :] = block
        twice_ref[length : 2 * length, :] = block
        return twice_ref[...]

    def late_inverse(slot, part):
        at = slice(half * part, half * part + half)
        if part < 2:
            ps[slot][at, :] = jnp.dot(inverse_ref[at, :], scaleds[slot][...], preferred_element_type=F32)

    def late_scan(i, slot, states, piece, pieces):
        for side in range(2):
            lane = 2 * i + side
            if piece == 0:
                states[side] = rate_rows(lane) + (jnp.zeros((8, 128), F32),)
            keep, keep_run, spread, state = states[side]
            for j in range(runs * piece // pieces, runs * (piece + 1) // pieces):
                at = slice(8 * j, 8 * j + 8)
                series = lead_ref[lane, at, :] + ps[slot][at, 128 * side : 128 * side + 128]
                force = weighted(series, own_ref[1, at, :], own_ref[2, at, :], spread)
                state = (own_ref[0, at, :] * keep) * state + force
                x_ref[lane, at, :] = state
            states[side] = (keep, keep_run, spread, state)
            if piece < pieces - 1:
                continue
            state, decay = over_runs(state, ends_ref[0] * keep_run)
            row = lax.broadcasted_iota(jnp.int32, (8, 128), 0)
            carry_ref[lane] = jnp.where(row == 0, 0.0, pltpu.roll(state, 1, 0))
            reach_ref[lane] = jnp.where(row == 0, 1.0, pltpu.roll(decay, 1, 0))

    def late_step(i, slot):
        step(i, slot, late_data(i + 1), late_inverse, late_scan)

    noise(sent_early).start()
    arrive(0)
    first_data = late_data(0)
    for part in range(4):
        forward(first_data, 0, part)
        scale(0, 0, part)

    def late_pair(u, carry):
        arrive(2 * u + 1)
        late_step(2 * u, 0)

        @pl.when(u == 0)
        def _():
            exchange_chips()
            noise(sent_early + 1).start()

        pl.when(u == 2)(exchange_groups)
        arrive(2 * u + 2)
        late_step(2 * u + 1, 1)
        return carry

    lax.fori_loop(0, chunks // 2 - 1, late_pair, 0)
    arrive(chunks - 1)
    late_step(chunks - 2, 0)
    states = [None, None]
    for part in range(2):
        late_inverse(1, part)
        late_scan(chunks - 2, 0, states, part, 2)
    exchange_back()
    whole(late_scan, chunks - 1, 1)
    give_copy.wait()
    incoming_ref[other_half, :] = take_ref[...]
    for lane in range(lanes):
        incoming = jnp.broadcast_to(incoming_ref[lane : lane + 1, :], (8, 128))
        x_ref[lane, length : length + 8, :] = carry_ref[lane] + reach_ref[lane] * incoming

    arrived(earlier_ref, noise_send.at[0])


def close(length, x_ref, out_hbm, stage_ref, sem):
    lanes = stage_ref.shape[0]
    runs = length // 8

    def out(lane):
        return pltpu.make_async_copy(
            stage_ref.at[lane], out_hbm.at[:, pl.ds(pl.multiple_of(lane * 128, 128), 128)], sem.at[lane]
        )

    def step(lane, carry):
        keep = jnp.exp(-jnp.broadcast_to(x_ref[lanes + 1, pl.ds(lane, 1), :], (8, 128)))
        state = x_ref[lane, length : length + 8, :] * keep
        for j in range(runs):
            at = slice(8 * j, 8 * j + 8)
            stage_ref[lane, pl.ds(j, 8, stride=runs), :] = x_ref[lane, at, :] + x_ref[lanes, at, :] * state
            state = state * keep
        out(lane).start()
        return carry

    lax.fori_loop(0, lanes, step, 0)

    def drain(lane, carry):
        out(lane).wait()
        return carry

    lax.fori_loop(0, lanes, drain, 0)


def shards(sections, random_forcing, eigen_root_table, lane_fading_speed, sudden_shrink):
    length, width = random_forcing.shape
    lanes, half = width // 128, length // 2
    chunk = 256
    chunks = width // chunk
    groups, chips = sections // MEMBERS, MEMBERS // 2
    forward, inverse = tables(length)
    hbm = pl.BlockSpec(memory_space=pltpu.HBM)
    vmem = pl.BlockSpec(memory_space=pltpu.VMEM)
    dma = pltpu.SemaphoreType.DMA
    tile = pltpu.VMEM((8, 128), F32)
    dense = pltpu.VMEM((lanes, 128), F32)
    x = pl.pallas_call(
        functools.partial(fields, length, sections),
        name="fields",
        out_shape=pltpu.VMEM((lanes + 2, length + 8, 128), F32),
        in_specs=[hbm] * 6,
        out_specs=vmem,
        scratch_shapes=[
            pltpu.VMEM((2 * length, width), BF16),
            pltpu.VMEM((lanes, 2 * length, 128), F32),
            pltpu.VMEM((2 * length, 2 * length), BF16),
            pltpu.VMEM((length, 6 * length), BF16),
            dense,
            pltpu.VMEM((length // 128, 128), F32),
            pltpu.VMEM((lanes, 3 * half, 128), F32),
            pltpu.VMEM((length, width), BF16),
            pltpu.VMEM((2 * length, chunk), BF16),
            pltpu.VMEM((2 * length, chunk), F32),
            pltpu.VMEM((2 * length, chunk), F32),
            pltpu.VMEM((6 * length, chunk), BF16),
            pltpu.VMEM((6 * length, chunk), BF16),
            pltpu.VMEM((length, chunk), F32),
            pltpu.VMEM((length, chunk), F32),
            pltpu.VMEM((length, chunk), F32),
            pltpu.VMEM((length, chunk), F32),
            pltpu.VMEM((lanes, length, 128), F32),
            pltpu.VMEM((3, length, 128), F32),
            pltpu.VMEM((3, length, 128), F32),
            tile,
            tile,
            pltpu.VMEM((2, 8, 128), F32),
            pltpu.VMEM((lanes, 8, 128), F32),
            pltpu.VMEM((lanes, 8, 128), F32),
            dense,
            pltpu.VMEM((1, 128), F32),
            dense,
            dense,
            pltpu.VMEM((2, 8, 128), F32),
            pltpu.VMEM((2, 8, 128), F32),
            pltpu.VMEM((3, 8, 128), F32),
            pltpu.VMEM((chips, 2, 8, 128), F32),
            pltpu.VMEM((groups, 2, 8, 128), F32),
            pltpu.VMEM((MEMBERS, 1, 128), F32),
            pltpu.VMEM((groups, 2, 128), F32),
            pltpu.VMEM((2, 128), F32),
            pltpu.VMEM((2, 8, 128), F32),
            pltpu.VMEM((2, 8, 128), F32),
            tile,
            tile,
            dma((5,)),
            dma((lanes // 4,)),
            dma((1,)),
            dma((chunks,)),
        ]
        + [dma((2,))] * 7,
        compiler_params=pltpu.CompilerParams(
            collective_id=0, has_side_effects=True, vmem_limit_bytes=44 * 2**20
        ),
    )(
        *(
            pltpu.with_memory_space_constraint(operand, pltpu.HBM)
            for operand in (
                random_forcing,
                eigen_root_table,
                jnp.asarray(forward),
                jnp.asarray(inverse),
                lane_fading_speed.reshape(lanes, 128),
                sudden_shrink.reshape(length // 128, 128),
            )
        )
    )
    return pl.pallas_call(
        functools.partial(close, length),
        name="close",
        out_shape=jax.ShapeDtypeStruct((length, width), F32),
        in_specs=[vmem],
        out_specs=hbm,
        scratch_shapes=[pltpu.VMEM((lanes, length, 128), F32), dma((lanes,))],
        compiler_params=pltpu.CompilerParams(vmem_limit_bytes=8 * 2**20),
    )(x)


def solution(mesh):
    return jax.shard_map(
        functools.partial(shards, mesh.shape["tm"]),
        mesh=mesh,
        in_specs=(P("tm", "chan"), P(None, "chan"), P("chan"), P("tm")),
        out_specs=P("tm", "chan"),
        check_vma=False,
    )
```

```python
import functools

import jax
import jax.numpy as jnp
import ml_dtypes
import numpy as np
from jax import lax
from jax.experimental import pallas as pl
from jax.experimental.pallas import tpu as pltpu
from jax.sharding import PartitionSpec as P

MESH = pl.DeviceIdType.MESH
F32 = jnp.float32
BF16 = jnp.bfloat16
MEMBERS = 16


def split(table):
    high = table.astype(ml_dtypes.bfloat16)
    low = (table - high.astype(np.float64)).astype(ml_dtypes.bfloat16)
    return high, low


@functools.lru_cache
def tables(length):
    half = length // 2
    t = np.arange(length)
    even = 2 * np.arange(half)
    odd = even + 1

    def basis(f, function):
        return function(2.0 * np.pi * (np.outer(f, t) % (2 * length)) / (2 * length))

    even_sine = basis(even, np.sin)
    even_sine[0] = np.cos(np.pi * t)
    rows = np.concatenate([basis(even, np.cos), even_sine, basis(odd, np.cos), basis(odd, np.sin)])
    forward = np.concatenate(split(rows), axis=1)
    runs = length // 8
    order = (np.arange(8)[None, :] * runs + np.arange(runs)[:, None]).reshape(-1)
    high, low = split(rows.T[order])
    parts = []
    for k in range(2):
        at = slice(k * length, (k + 1) * length)
        parts += [high[:, at], low[:, at]]
    return forward, np.concatenate(parts, axis=1)


def flipped(tile):
    at = 7 - lax.broadcasted_iota(jnp.int32, tile.shape, 0)
    return jnp.take_along_axis(tile, at, axis=0)


def fold(e_ref, es_ref, lane, length, piece, pieces):
    half = length // 2
    scale = 1.0 / (2 * length)
    row = lax.broadcasted_iota(jnp.int32, (8, 128), 0)
    blocks = half // 8
    for b in range(blocks * piece // pieces, blocks * (piece + 1) // pieces):
        value = e_ref[lane, pl.ds(16 * b, 8, stride=2), :]
        if b:
            mirror = flipped(e_ref[lane, pl.ds(2 * length - 14 - 16 * b, 8, stride=2), :])
        else:
            mirror = flipped(e_ref[lane, pl.ds(2 * length - 16, 8, stride=2), :])
            mirror = jnp.where(row == 0, 0.0, pltpu.roll(mirror, 1, 0))
        total = (value + mirror) * scale
        es_ref[lane, 8 * b : 8 * b + 8, :] = total
        if b == 0:
            middle = jnp.broadcast_to(e_ref[lane, length : length + 1, :], (8, 128)) * scale
            total = jnp.where(row == 0, middle, total)
        es_ref[lane, half + 8 * b : half + 8 * b + 8, :] = total
        value = e_ref[lane, pl.ds(16 * b + 1, 8, stride=2), :]
        mirror = flipped(e_ref[lane, pl.ds(2 * length - 15 - 16 * b, 8, stride=2), :])
        es_ref[lane, 2 * half + 8 * b : 2 * half + 8 * b + 8, :] = (value + mirror) * -scale


def over_runs(state, decay):
    row = lax.broadcasted_iota(jnp.int32, state.shape, 0)
    for step in (1, 2, 4):
        reach = row >= step
        state = jnp.where(reach, decay * pltpu.roll(state, step, 0) + state, state)
        decay = jnp.where(reach, decay * pltpu.roll(decay, step, 0), decay)
    return state, decay


def weighted(value, loss, power, spread):
    square = loss + power * spread
    return square * lax.rsqrt(square) * value


def spread_of(rate):
    x = 2.0 * rate
    series = 1.0 - x * (1.0 / 6.0)
    for k in (5, 4, 3, 2):
        series = 1.0 - x * (1.0 / k) * series
    return x * series


def fields(
    length, sections, v_hbm, e_hbm, forward_hbm, inverse_hbm, rate_hbm, burst_hbm, x_ref,
    v_ref, e_ref, forward_ref, inverse_ref, rate_ref, burst_line, es_ref, earlier_ref, twice_ref,
    value0_ref, value1_ref, scaled0_ref, scaled1_ref, p0_ref, p1_ref, q0_ref, q1_ref, lead_ref,
    own_ref, next_ref, burst_ref, next_burst_ref, ends_ref, carry_ref, reach_ref, incoming_ref, logs_ref,
    a_ref, c_ref, pair_out_ref, pair_in_ref, before_ref, chips_ref, groups_ref,
    member_logs_ref, group_logs_ref, group_log_ref, chip_out_ref, group_out_ref, give_ref, take_ref,
    t_sem, e_sem, noise_send, noise_recv, burst_sem, pair_sem, give_sem, logs_sem, chips_sem, groups_sem, glogs_sem,
):
    width = v_hbm.shape[1]
    chunk = 256
    chunks = width // chunk
    lanes = width // 128
    half = length // 2
    runs = length // 8
    groups = sections // MEMBERS
    chips = MEMBERS // 2
    me = lax.axis_index("tm")
    group, member = me // MEMBERS, me % MEMBERS
    chip, core = member // 2, member % 2
    after, before = (me + 1) % sections, (me + sections - 1) % sections
    partner = group * MEMBERS + chip * 2 + (1 - core)
    values, scaleds = (value0_ref, value1_ref), (scaled0_ref, scaled1_ref)
    ps, qs = (p0_ref, p1_ref), (q0_ref, q1_ref)

    def remote(source, target, send, recv, device):
        return pltpu.make_async_remote_copy(
            src_ref=source, dst_ref=target, send_sem=send, recv_sem=recv, device_id={"tm": device}, device_id_type=MESH
        )

    def columns(i):
        return pl.ds(pl.multiple_of(i * chunk, chunk), chunk)

    members = [group * MEMBERS + (member + k) % MEMBERS for k in range(1, MEMBERS)]
    chip_peers = [group * MEMBERS + ((chip + k) % chips) * 2 + core for k in range(1, chips)]
    group_peers = [((group + k) % groups) * MEMBERS + member for k in range(1, groups)]

    barrier = pltpu.get_barrier_semaphore()
    for device in [after, before] + group_peers + members:
        pl.semaphore_signal(barrier, inc=1, device_id={"tm": device}, device_id_type=MESH)

    def arrived(ref, sem):
        pltpu.make_async_copy(ref, ref, sem).wait()

    def table(lane):
        return pltpu.make_async_copy(e_hbm.at[:, pl.ds(lane * 128, 128)], e_ref.at[lane], e_sem.at[lane // 4])

    for lane in range(4):
        table(lane).start()
    pltpu.make_async_copy(burst_hbm, burst_line, t_sem.at[0]).start()
    pltpu.make_async_copy(rate_hbm, rate_ref, t_sem.at[4]).start()
    pltpu.make_async_copy(v_hbm, v_ref, t_sem.at[1]).start()
    pltpu.make_async_copy(forward_hbm, forward_ref, t_sem.at[2]).start()
    for k, source in enumerate((0, 0, 1, 2, 2, 3)):
        pltpu.make_async_copy(
            inverse_hbm.at[:, pl.ds(source * length, length)], inverse_ref.at[:, pl.ds(k * length, length)], t_sem.at[3]
        ).start()

    def broadcasts(source_ref, target_ref):
        product = jnp.ones((8, 128), F32)
        for j in range(runs):
            column = jnp.broadcast_to(source_ref[:, j : j + 1], (8, 128))
            at = slice(8 * j, 8 * j + 8)
            power = column * column
            target_ref[0, at, :] = column
            target_ref[1, at, :] = 1.0 - power
            target_ref[2, at, :] = power
            product = product * column
            if source_ref is burst_ref:
                x_ref[lanes, 8 * j : 8 * j + 8, :] = product
        return product

    def noise(i):
        return remote(v_hbm.at[:, columns(i)], earlier_ref.at[:, columns(i)], noise_send.at[0], noise_recv.at[i], after)

    burst_copy = remote(burst_ref, next_burst_ref, burst_sem.at[0], burst_sem.at[1], before)

    def fold_step(lane, carry):
        fold(e_ref, es_ref, lane, length, 0, 1)
        return carry

    arrived(burst_line, t_sem.at[0])
    line = jnp.concatenate([burst_line[k : k + 1, :] for k in range(length // 128)], axis=1)
    burst_ref[:, 0:runs] = jnp.concatenate([line[:, runs * k : runs * k + runs] for k in range(8)], axis=0)
    burst_ref[:, runs:128] = jnp.ones((8, 128 - runs), F32)
    logs_ref[...] = jnp.broadcast_to(jnp.sum(jnp.log(line), axis=1, keepdims=True), (1, 128))

    pl.semaphore_wait(barrier, 2 + (MEMBERS - 1) + (groups - 1))
    burst_copy.start()
    for device in members:
        remote(logs_ref, member_logs_ref.at[member], logs_sem.at[0], logs_sem.at[1], device).start()
    for i in range(4):
        noise(i).start()
    for lane in range(4, 8):
        table(lane).start()

    ends_ref[0] = broadcasts(burst_ref, own_ref)
    arrived(e_ref.at[pl.ds(0, 4)], e_sem.at[0])
    lax.fori_loop(0, 4, fold_step, 0)
    for k, ref in ((4, rate_ref), (1, v_ref), (2, forward_ref)):
        arrived(ref, t_sem.at[k])
    x_ref[lanes + 1, 0:lanes, :] = rate_ref[...]

    def rate_rows(lane):
        rate = jnp.broadcast_to(rate_ref[pl.ds(lane, 1), :], (8, 128))
        return jnp.exp(-rate), jnp.exp(-runs * rate), spread_of(rate)

    def doubled(source_ref, i):
        block = source_ref[:, columns(i)]
        twice_ref[0:length, :] = block
        twice_ref[length : 2 * length, :] = block
        return twice_ref[...]

    def forward(data, slot, part):
        at = slice(half * part, half * part + half)
        values[slot][at, :] = jnp.dot(forward_ref[at, :], data, preferred_element_type=F32)

    def scale(i, slot, part):
        at = (0, half, 2 * half, 2 * half)[part]
        base = 3 * length * (part // 2) + half * (part % 2)
        for side in range(2):
            cut = slice(128 * side, 128 * side + 128)
            scaled = values[slot][half * part : half * part + half, cut] * es_ref[2 * i + side, at : at + half, :]
            high = scaled.astype(BF16)
            low = (scaled - high.astype(F32)).astype(BF16)
            scaleds[slot][base : base + half, cut] = high
            scaleds[slot][base + length : base + length + half, cut] = low
            scaleds[slot][base + 2 * length : base + 2 * length + half, cut] = high

    def early_inverse(slot, part):
        target, cut = (ps, qs)[part // 2], slice(3 * length * (part // 2), 3 * length * (part // 2) + 3 * length)
        at = slice(half * (part % 2), half * (part % 2) + half)
        target[slot][at, :] = jnp.dot(inverse_ref[at, cut], scaleds[slot][cut, :], preferred_element_type=F32)

    def early_scan(i, slot, states, piece, pieces):
        for side in range(2):
            lane = 2 * i + side
            if piece == 0:
                states[side] = rate_rows(lane) + (jnp.zeros((8, 128), F32), jnp.zeros((8, 128), F32))
            keep, keep_run, spread, here, there = states[side]
            for j in range(runs * piece // pieces, runs * (piece + 1) // pieces):
                at = slice(8 * j, 8 * j + 8)
                p = ps[slot][at, 128 * side : 128 * side + 128]
                q = qs[slot][at, 128 * side : 128 * side + 128]
                lead = p - q
                lead_ref[lane, at, :] = lead
                force = weighted(lead, own_ref[1, at, :], own_ref[2, at, :], spread)
                here = (own_ref[0, at, :] * keep) * here + force
                force = weighted(p + q, next_ref[1, at, :], next_ref[2, at, :], spread)
                there = (next_ref[0, at, :] * keep) * there + force
            states[side] = (keep, keep_run, spread, here, there)
            if piece < pieces - 1:
                continue
            here, _ = over_runs(here, ends_ref[0] * keep_run)
            there, _ = over_runs(there, ends_ref[1] * keep_run)
            a_ref[pl.ds(lane, 1), :] = here[7:8, :]
            c_ref[pl.ds(lane, 1), :] = there[7:8, :]

    def whole(scan, i, slot):
        scan(i, slot, [None, None], 0, 1)

    def step(i, slot, data, inverse, scan, folding=None):
        states = [None, None]
        for part in range(4):
            forward(data, 1 - slot, part)
            scan((i + chunks - 1) % chunks, 1 - slot, states, part, 8)
            if folding is not None:
                fold(e_ref, es_ref, folding, length, part, 4)
        for part in range(4):
            inverse(slot, part)
            scale(i + 1, 1 - slot, part)
            scan((i + chunks - 1) % chunks, 1 - slot, states, part + 4, 8)
            if folding is not None:
                fold(e_ref, es_ref, folding + 1, length, part, 4)

    def early_step(i, slot, folding=None):
        step(i, slot, doubled(v_ref, i + 1), early_inverse, early_scan, folding)

    first_data = doubled(v_ref, 0)
    for part in range(4):
        forward(first_data, 0, part)
        scale(0, 0, part)
    arrived(inverse_ref, t_sem.at[3])
    def early_pair(u, carry):
        noise(4 + u).start()
        arrived(e_ref.at[pl.ds(pl.multiple_of(4 * u + 4, 4), 4)], e_sem.at[u + 1])

        @pl.when(u == 0)
        def _():
            for lane in range(8, lanes):
                table(lane).start()

        early_step(2 * u, 0, 4 * u + 4)

        early_step(2 * u + 1, 1, 4 * u + 6)

        @pl.when(u == 0)
        def _():
            burst_copy.wait()
            ends_ref[1] = broadcasts(next_burst_ref, next_ref)
            whole(early_scan, 0, 0)

        return carry

    lax.fori_loop(0, chunks // 2 - 1, early_pair, 0)
    early_step(chunks - 2, 0)
    states = [None, None]
    for part in range(4):
        early_inverse(1, part)
        early_scan(chunks - 2, 0, states, part, 4)
    whole(early_scan, chunks - 1, 1)
    sent_early = chunks // 2 + 3

    own_half = pl.ds(pl.multiple_of(core * 8, 8), 8)
    other_half = pl.ds(pl.multiple_of((1 - core) * 8, 8), 8)
    pair_copy = remote(pair_out_ref, pair_in_ref, pair_sem.at[0], pair_sem.at[1], partner)
    give_copy = remote(give_ref, take_ref, give_sem.at[0], give_sem.at[1], partner)
    pair_out_ref[0] = a_ref[other_half, :]
    pair_out_ref[1] = c_ref[other_half, :]
    pair_copy.start()

    for k in range(2):
        arrived(member_logs_ref.at[pl.ds(0, MEMBERS - 1)], logs_sem.at[k])
    member_logs_ref[pl.ds(member, 1)] = logs_ref[...].reshape(1, 1, 128)
    logs_of = [member_logs_ref[k] for k in range(MEMBERS)]
    group_log_ref[0:1, :] = sum(logs_of[1:], logs_of[0])
    group_log_ref[1:2, :] = logs_of[0]
    group_logs_ref[pl.ds(group, 1)] = group_log_ref[...].reshape(1, 2, 128)
    for device in group_peers:
        remote(group_log_ref, group_logs_ref.at[group], glogs_sem.at[0], glogs_sem.at[1], device).start()

    def log_of(index):
        return jnp.broadcast_to(member_logs_ref[index], (8, 128)) - length * rate_ref[own_half, :]

    def of_first(k):
        own = (a_ref, c_ref)[k][own_half, :]
        return jnp.where(core == 0, own, pair_in_ref[k])

    def of_second(k):
        own = (a_ref, c_ref)[k][own_half, :]
        return jnp.where(core == 0, pair_in_ref[k], own)

    def exchange_chips():
        pair_copy.wait()
        chip_out_ref[0] = jnp.exp(log_of(2 * chip + 1)) * of_first(0) + of_first(1) + of_second(0)
        chip_out_ref[1] = of_second(1)
        for device in chip_peers:
            remote(chip_out_ref, chips_ref.at[chip], chips_sem.at[0], chips_sem.at[1], device).start()
        chips_ref[pl.ds(chip, 1)] = chip_out_ref[...].reshape(1, 2, 8, 128)

    def exchange_groups():
        for k in range(2):
            arrived(chips_ref.at[pl.ds(0, chips - 1)], chips_sem.at[k])
        state = jnp.zeros((8, 128), F32)
        log, tail = state, state
        before = (state, log, tail)
        for k in range(chips):
            here = chip == k
            before = tuple(jnp.where(here, new, old) for new, old in zip((state, log, tail), before))
            second = log_of(2 * k + 1)
            step = log_of(2 * k) + second
            state = jnp.exp(step) * state + jnp.exp(second) * tail + chips_ref[k, 0]
            tail = chips_ref[k, 1]
            log = log + step
        group_out_ref[0] = state
        group_out_ref[1] = tail
        for device in group_peers:
            remote(group_out_ref, groups_ref.at[group], groups_sem.at[0], groups_sem.at[1], device).start()
        groups_ref[pl.ds(group, 1)] = group_out_ref[...].reshape(1, 2, 8, 128)
        for k in range(3):
            before_ref[k] = before[k]

    def exchange_back():
        for k in range(2):
            arrived(groups_ref.at[pl.ds(0, groups - 1)], groups_sem.at[k])
        for k in range(2):
            arrived(group_logs_ref.at[pl.ds(0, groups - 1)], glogs_sem.at[k])
        rate = rate_ref[own_half, :]
        entering = groups_ref[(group + groups - 1) % groups, 1]
        state = jnp.zeros((8, 128), F32)
        log, tail = state, entering
        for k in range(groups):
            at = (group + k) % groups
            total = jnp.broadcast_to(group_logs_ref[at, 0:1, :], (8, 128))
            first = jnp.broadcast_to(group_logs_ref[at, 1:2, :], (8, 128))
            step = total - (MEMBERS * length) * rate
            rest = (total - first) - ((MEMBERS - 1) * length) * rate
            state = jnp.exp(step) * state + jnp.exp(rest) * tail + groups_ref[at, 0]
            tail = groups_ref[at, 1]
            log = log + step
        opening = state / (1.0 - jnp.exp(log))
        log = before_ref[1]
        arriving = jnp.where(chip == 0, 0.0, jnp.exp(log - log_of(0)) * entering)
        first_in = jnp.exp(log) * opening + before_ref[0] + arriving
        tail = jnp.where(chip == 0, entering, before_ref[2])
        second_in = jnp.exp(log_of(2 * chip)) * first_in + of_first(0) + tail
        incoming_ref[own_half, :] = jnp.where(core == 0, first_in, second_in)
        give_ref[...] = jnp.where(core == 0, second_in, first_in)
        give_copy.start()

    def arrive(i):
        noise(i).wait_recv()

    def late_inverse(slot, part):
        at = slice(half * part, half * part + half)
        if part < 2:
            ps[slot][at, :] = jnp.dot(inverse_ref[at, :], scaleds[slot][...], preferred_element_type=F32)

    def late_scan(i, slot, states, piece, pieces):
        for side in range(2):
            lane = 2 * i + side
            if piece == 0:
                states[side] = rate_rows(lane) + (jnp.zeros((8, 128), F32),)
            keep, keep_run, spread, state = states[side]
            for j in range(runs * piece // pieces, runs * (piece + 1) // pieces):
                at = slice(8 * j, 8 * j + 8)
                series = lead_ref[lane, at, :] + ps[slot][at, 128 * side : 128 * side + 128]
                force = weighted(series, own_ref[1, at, :], own_ref[2, at, :], spread)
                state = (own_ref[0, at, :] * keep) * state + force
                x_ref[lane, at, :] = state
            states[side] = (keep, keep_run, spread, state)
            if piece < pieces - 1:
                continue
            state, decay = over_runs(state, ends_ref[0] * keep_run)
            row = lax.broadcasted_iota(jnp.int32, (8, 128), 0)
            carry_ref[lane] = jnp.where(row == 0, 0.0, pltpu.roll(state, 1, 0))
            reach_ref[lane] = jnp.where(row == 0, 1.0, pltpu.roll(decay, 1, 0))

    def late_step(i, slot):
        step(i, slot, doubled(earlier_ref, i + 1), late_inverse, late_scan)

    arrive(0)
    first_data = doubled(earlier_ref, 0)
    for part in range(4):
        forward(first_data, 0, part)
        scale(0, 0, part)

    def late_pair(u, carry):
        arrive(2 * u + 1)
        late_step(2 * u, 0)

        @pl.when(u == 0)
        def _():
            exchange_chips()
            noise(sent_early).start()

        pl.when(u == 2)(exchange_groups)
        arrive(2 * u + 2)
        late_step(2 * u + 1, 1)
        return carry

    lax.fori_loop(0, chunks // 2 - 1, late_pair, 0)
    states = [None, None]
    for part in range(2):
        late_inverse(0, part)
        late_scan(chunks - 3, 1, states, part, 2)
    whole(late_scan, chunks - 2, 0)
    arrive(chunks - 1)
    last_data = doubled(earlier_ref, chunks - 1)
    for part in range(4):
        forward(last_data, 1, part)
        scale(chunks - 1, 1, part)
    exchange_back()
    states = [None, None]
    for part in range(2):
        late_inverse(1, part)
    for part in range(2):
        late_scan(chunks - 1, 1, states, part, 2)
    give_copy.wait()
    incoming_ref[other_half, :] = take_ref[...]
    for lane in range(lanes):
        incoming = jnp.broadcast_to(incoming_ref[lane : lane + 1, :], (8, 128))
        x_ref[lane, length : length + 8, :] = carry_ref[lane] + reach_ref[lane] * incoming

    arrived(earlier_ref, noise_send.at[0])


def close(length, x_ref, out_hbm, stage_ref, sem):
    lanes = stage_ref.shape[0]
    runs = length // 8
    spread_ref = stage_ref.reshape(lanes, 8 * (runs + 8), 128)

    def out(lane):
        return pltpu.make_async_copy(
            stage_ref.at[lane, :, pl.ds(0, runs)],
            out_hbm.at[:, :, pl.ds(pl.multiple_of(lane * 128, 128), 128)],
            sem.at[0],
        )

    def step(pair, carry):
        both = (2 * pair, 2 * pair + 1)
        keep = [jnp.exp(-jnp.broadcast_to(x_ref[lanes + 1, pl.ds(lane, 1), :], (8, 128))) for lane in both]
        state = [x_ref[lane, length : length + 8, :] * k for lane, k in zip(both, keep)]
        for j in range(runs):
            at = slice(8 * j, 8 * j + 8)
            grown = x_ref[lanes, at, :]
            for side, lane in enumerate(both):
                spread_ref[lane, pl.ds(j, 8, stride=runs + 8), :] = x_ref[lane, at, :] + grown * state[side]
                state[side] = state[side] * keep[side]
        for lane in both:
            out(lane).start()
        return carry

    lax.fori_loop(0, lanes // 2, step, 0)

    written = stage_ref.at[:, :, pl.ds(0, runs)]
    pltpu.make_async_copy(written, written, sem.at[0]).wait()


def shards(sections, random_forcing, eigen_root_table, lane_fading_speed, sudden_shrink):
    length, width = random_forcing.shape
    lanes, half = width // 128, length // 2
    chunk = 256
    chunks = width // chunk
    groups, chips = sections // MEMBERS, MEMBERS // 2
    forward, inverse = tables(length)
    hbm = pl.BlockSpec(memory_space=pltpu.HBM)
    vmem = pl.BlockSpec(memory_space=pltpu.VMEM)
    dma = pltpu.SemaphoreType.DMA
    tile = pltpu.VMEM((8, 128), F32)
    dense = pltpu.VMEM((lanes, 128), F32)
    x = pl.pallas_call(
        functools.partial(fields, length, sections),
        name="fields",
        out_shape=pltpu.VMEM((lanes + 2, length + 8, 128), F32),
        in_specs=[hbm] * 6,
        out_specs=vmem,
        scratch_shapes=[
            pltpu.VMEM((length, width), BF16),
            pltpu.VMEM((lanes, 2 * length, 128), F32),
            pltpu.VMEM((2 * length, 2 * length), BF16),
            pltpu.VMEM((length, 6 * length), BF16),
            dense,
            pltpu.VMEM((length // 128, 128), F32),
            pltpu.VMEM((lanes, 3 * half, 128), F32),
            pltpu.VMEM((length, width), BF16),
            pltpu.VMEM((2 * length, chunk), BF16),
            pltpu.VMEM((2 * length, chunk), F32),
            pltpu.VMEM((2 * length, chunk), F32),
            pltpu.VMEM((6 * length, chunk), BF16),
            pltpu.VMEM((6 * length, chunk), BF16),
            pltpu.VMEM((length, chunk), F32),
            pltpu.VMEM((length, chunk), F32),
            pltpu.VMEM((length, chunk), F32),
            pltpu.VMEM((length, chunk), F32),
            pltpu.VMEM((lanes, length, 128), F32),
            pltpu.VMEM((3, length, 128), F32),
            pltpu.VMEM((3, length, 128), F32),
            tile,
            tile,
            pltpu.VMEM((2, 8, 128), F32),
            pltpu.VMEM((lanes, 8, 128), F32),
            pltpu.VMEM((lanes, 8, 128), F32),
            dense,
            pltpu.VMEM((1, 128), F32),
            dense,
            dense,
            pltpu.VMEM((2, 8, 128), F32),
            pltpu.VMEM((2, 8, 128), F32),
            pltpu.VMEM((3, 8, 128), F32),
            pltpu.VMEM((chips, 2, 8, 128), F32),
            pltpu.VMEM((groups, 2, 8, 128), F32),
            pltpu.VMEM((MEMBERS, 1, 128), F32),
            pltpu.VMEM((groups, 2, 128), F32),
            pltpu.VMEM((2, 128), F32),
            pltpu.VMEM((2, 8, 128), F32),
            pltpu.VMEM((2, 8, 128), F32),
            tile,
            tile,
            dma((5,)),
            dma((lanes // 4,)),
            dma((1,)),
            dma((chunks,)),
        ]
        + [dma((2,))] * 7,
        compiler_params=pltpu.CompilerParams(
            collective_id=0, has_side_effects=True, vmem_limit_bytes=44 * 2**20
        ),
    )(
        *(
            pltpu.with_memory_space_constraint(operand, pltpu.HBM)
            for operand in (
                random_forcing,
                eigen_root_table,
                jnp.asarray(forward),
                jnp.asarray(inverse),
                lane_fading_speed.reshape(lanes, 128),
                sudden_shrink.reshape(length // 128, 128),
            )
        )
    )
    return pl.pallas_call(
        functools.partial(close, length),
        name="close",
        out_shape=jax.ShapeDtypeStruct((8, length // 8, width), F32),
        in_specs=[vmem],
        out_specs=hbm,
        scratch_shapes=[pltpu.VMEM((lanes, 8, length // 8 + 8, 128), F32), dma((1,))],
        compiler_params=pltpu.CompilerParams(vmem_limit_bytes=8 * 2**20),
    )(x).reshape(length, width)


def solution(mesh):
    return jax.shard_map(
        functools.partial(shards, mesh.shape["tm"]),
        mesh=mesh,
        in_specs=(P("tm", "chan"), P(None, "chan"), P("chan"), P("tm")),
        out_specs=P("tm", "chan"),
        check_vma=False,
    )
```

```python
import functools

import jax
import jax.numpy as jnp
import ml_dtypes
import numpy as np
from jax import lax
from jax.experimental import pallas as pl
from jax.experimental.pallas import tpu as pltpu
from jax.sharding import PartitionSpec as P

MESH = pl.DeviceIdType.MESH
F32 = jnp.float32
BF16 = jnp.bfloat16
MEMBERS = 16


def split(table):
    high = table.astype(ml_dtypes.bfloat16)
    low = (table - high.astype(np.float64)).astype(ml_dtypes.bfloat16)
    return high, low


@functools.lru_cache
def tables(length):
    half = length // 2
    t = np.arange(length)
    even = 2 * np.arange(half)
    odd = even + 1

    def basis(f, function):
        return function(2.0 * np.pi * (np.outer(f, t) % (2 * length)) / (2 * length))

    even_sine = basis(even, np.sin)
    even_sine[0] = np.cos(np.pi * t)
    rows = np.concatenate([basis(even, np.cos), even_sine, basis(odd, np.cos), basis(odd, np.sin)])
    forward = np.concatenate(split(rows), axis=1)
    runs = length // 8
    order = (np.arange(8)[None, :] * runs + np.arange(runs)[:, None]).reshape(-1)
    high, low = split(rows.T[order])
    parts = []
    for k in range(2):
        at = slice(k * length, (k + 1) * length)
        parts += [high[:, at], low[:, at]]
    return forward, np.concatenate(parts, axis=1)


def flipped(tile):
    at = 7 - lax.broadcasted_iota(jnp.int32, tile.shape, 0)
    return jnp.take_along_axis(tile, at, axis=0)


def fold(e_ref, es_ref, lane, length, piece, pieces):
    half = length // 2
    scale = 1.0 / (2 * length)
    row = lax.broadcasted_iota(jnp.int32, (8, 128), 0)
    blocks = half // 8
    for b in range(blocks * piece // pieces, blocks * (piece + 1) // pieces):
        value = e_ref[lane, pl.ds(16 * b, 8, stride=2), :]
        if b:
            mirror = flipped(e_ref[lane, pl.ds(2 * length - 14 - 16 * b, 8, stride=2), :])
        else:
            mirror = flipped(e_ref[lane, pl.ds(2 * length - 16, 8, stride=2), :])
            mirror = jnp.where(row == 0, 0.0, pltpu.roll(mirror, 1, 0))
        total = (value + mirror) * scale
        es_ref[lane, 8 * b : 8 * b + 8, :] = total
        if b == 0:
            middle = jnp.broadcast_to(e_ref[lane, length : length + 1, :], (8, 128)) * scale
            total = jnp.where(row == 0, middle, total)
        es_ref[lane, half + 8 * b : half + 8 * b + 8, :] = total
        value = e_ref[lane, pl.ds(16 * b + 1, 8, stride=2), :]
        mirror = flipped(e_ref[lane, pl.ds(2 * length - 15 - 16 * b, 8, stride=2), :])
        es_ref[lane, 2 * half + 8 * b : 2 * half + 8 * b + 8, :] = (value + mirror) * -scale


def over_runs(state, decay):
    row = lax.broadcasted_iota(jnp.int32, state.shape, 0)
    for step in (1, 2, 4):
        reach = row >= step
        state = jnp.where(reach, decay * pltpu.roll(state, step, 0) + state, state)
        decay = jnp.where(reach, decay * pltpu.roll(decay, step, 0), decay)
    return state, decay


def weighted(value, loss, power, spread):
    square = loss + power * spread
    return square * lax.rsqrt(square) * value


def spread_of(rate):
    x = 2.0 * rate
    series = 1.0 - x * (1.0 / 6.0)
    for k in (5, 4, 3, 2):
        series = 1.0 - x * (1.0 / k) * series
    return x * series


def fields(
    length, sections, v_hbm, e_hbm, forward_hbm, inverse_hbm, rate_hbm, burst_hbm, x_ref,
    v_ref, e_ref, forward_ref, inverse_ref, rate_ref, burst_line, es_ref, earlier_ref, twice_ref,
    value0_ref, value1_ref, scaled0_ref, scaled1_ref, p0_ref, p1_ref, q0_ref, q1_ref, tails_ref, lead_ref,
    own_ref, next_ref, burst_ref, next_burst_ref, ends_ref, carry_ref, reach_ref, incoming_ref, logs_ref,
    a_ref, c_ref, pair_out_ref, pair_in_ref, before_ref, chips_ref, groups_ref,
    member_logs_ref, group_logs_ref, group_log_ref, chip_out_ref, group_out_ref, give_ref, take_ref,
    t_sem, e_sem, noise_send, noise_recv, burst_sem, pair_sem, give_sem, logs_sem, chips_sem, groups_sem, glogs_sem,
):
    width = v_hbm.shape[1]
    chunk = 256
    chunks = width // chunk
    lanes = width // 128
    half = length // 2
    runs = length // 8
    groups = sections // MEMBERS
    chips = MEMBERS // 2
    me = lax.axis_index("tm")
    group, member = me // MEMBERS, me % MEMBERS
    chip, core = member // 2, member % 2
    after, before = (me + 1) % sections, (me + sections - 1) % sections
    partner = group * MEMBERS + chip * 2 + (1 - core)
    values, scaleds = (value0_ref, value1_ref), (scaled0_ref, scaled1_ref)
    ps, qs = (p0_ref, p1_ref), (q0_ref, q1_ref)

    def remote(source, target, send, recv, device):
        return pltpu.make_async_remote_copy(
            src_ref=source, dst_ref=target, send_sem=send, recv_sem=recv, device_id={"tm": device}, device_id_type=MESH
        )

    def columns(i):
        return pl.ds(pl.multiple_of(i * chunk, chunk), chunk)

    members = [group * MEMBERS + (member + k) % MEMBERS for k in range(1, MEMBERS)]
    chip_peers = [group * MEMBERS + ((chip + k) % chips) * 2 + core for k in range(1, chips)]
    group_peers = [((group + k) % groups) * MEMBERS + member for k in range(1, groups)]

    barrier = pltpu.get_barrier_semaphore()
    for device in [after, before] + group_peers + members:
        pl.semaphore_signal(barrier, inc=1, device_id={"tm": device}, device_id_type=MESH)

    def arrived(ref, sem):
        pltpu.make_async_copy(ref, ref, sem).wait()

    def table(lane):
        return pltpu.make_async_copy(e_hbm.at[:, pl.ds(lane * 128, 128)], e_ref.at[lane], e_sem.at[lane // 4])

    for lane in range(4):
        table(lane).start()
    pltpu.make_async_copy(burst_hbm, burst_line, t_sem.at[0]).start()
    pltpu.make_async_copy(rate_hbm, rate_ref, t_sem.at[4]).start()
    pltpu.make_async_copy(v_hbm, v_ref, t_sem.at[1]).start()
    pltpu.make_async_copy(forward_hbm, forward_ref, t_sem.at[2]).start()
    for k, source in enumerate((0, 0, 1, 2, 2, 3)):
        pltpu.make_async_copy(
            inverse_hbm.at[:, pl.ds(source * length, length)], inverse_ref.at[:, pl.ds(k * length, length)], t_sem.at[3]
        ).start()

    def broadcasts(source_ref, target_ref):
        product = jnp.ones((8, 128), F32)
        for j in range(runs):
            column = jnp.broadcast_to(source_ref[:, j : j + 1], (8, 128))
            at = slice(8 * j, 8 * j + 8)
            power = column * column
            target_ref[0, at, :] = column
            target_ref[1, at, :] = 1.0 - power
            target_ref[2, at, :] = power
            product = product * column
            if source_ref is burst_ref:
                x_ref[lanes, 8 * j : 8 * j + 8, :] = product
        return product

    def noise(i):
        return remote(v_hbm.at[:, columns(i)], earlier_ref.at[:, columns(i)], noise_send.at[0], noise_recv.at[i], after)

    burst_copy = remote(burst_ref, next_burst_ref, burst_sem.at[0], burst_sem.at[1], before)

    def fold_step(lane, carry):
        fold(e_ref, es_ref, lane, length, 0, 1)
        return carry

    arrived(burst_line, t_sem.at[0])
    line = jnp.concatenate([burst_line[k : k + 1, :] for k in range(length // 128)], axis=1)
    burst_ref[:, 0:runs] = jnp.concatenate([line[:, runs * k : runs * k + runs] for k in range(8)], axis=0)
    burst_ref[:, runs:128] = jnp.ones((8, 128 - runs), F32)
    logs_ref[...] = jnp.broadcast_to(jnp.sum(jnp.log(line), axis=1, keepdims=True), (1, 128))

    def meet():
        pl.semaphore_wait(barrier, 2 + (MEMBERS - 1) + (groups - 1))
        burst_copy.start()
        for device in members:
            remote(logs_ref, member_logs_ref.at[member], logs_sem.at[0], logs_sem.at[1], device).start()
        for i in range(4):
            noise(i).start()

    pl.when(chip >= chips // 2)(meet)
    for lane in range(4, 8):
        table(lane).start()
    ends_ref[0] = broadcasts(burst_ref, own_ref)
    arrived(e_ref.at[pl.ds(0, 4)], e_sem.at[0])
    lax.fori_loop(0, 4, fold_step, 0)
    for k, ref in ((4, rate_ref), (1, v_ref), (2, forward_ref)):
        arrived(ref, t_sem.at[k])
    x_ref[lanes + 1, 0:lanes, :] = rate_ref[...]

    def rate_rows(lane):
        rate = jnp.broadcast_to(rate_ref[pl.ds(lane, 1), :], (8, 128))
        return jnp.exp(-rate), jnp.exp(-runs * rate), spread_of(rate)

    def doubled(source_ref, i):
        block = source_ref[:, columns(i)]
        twice_ref[0:length, :] = block
        twice_ref[length : 2 * length, :] = block
        return twice_ref[...]

    def forward(data, slot, part):
        at = slice(half * part, half * part + half)
        values[slot][at, :] = jnp.dot(forward_ref[at, :], data, preferred_element_type=F32)

    def scale(i, slot, part):
        at = (0, half, 2 * half, 2 * half)[part]
        base = 3 * length * (part // 2) + half * (part % 2)
        for side in range(2):
            cut = slice(128 * side, 128 * side + 128)
            scaled = values[slot][half * part : half * part + half, cut] * es_ref[2 * i + side, at : at + half, :]
            high = scaled.astype(BF16)
            low = (scaled - high.astype(F32)).astype(BF16)
            scaleds[slot][base : base + half, cut] = high
            scaleds[slot][base + length : base + length + half, cut] = low
            scaleds[slot][base + 2 * length : base + 2 * length + half, cut] = high

    def early_inverse(slot, part):
        target, cut = (ps, qs)[part // 2], slice(3 * length * (part // 2), 3 * length * (part // 2) + 3 * length)
        at = slice(half * (part % 2), half * (part % 2) + half)
        target[slot][at, :] = jnp.dot(inverse_ref[at, cut], scaleds[slot][cut, :], preferred_element_type=F32)

    def early_scan(i, slot, states, piece, pieces):
        for side in range(2):
            lane = 2 * i + side
            if piece == 0:
                states[side] = rate_rows(lane) + (jnp.zeros((8, 128), F32), jnp.zeros((8, 128), F32))
            keep, keep_run, spread, here, there = states[side]
            for j in range(runs * piece // pieces, runs * (piece + 1) // pieces):
                at = slice(8 * j, 8 * j + 8)
                p = ps[slot][at, 128 * side : 128 * side + 128]
                q = qs[slot][at, 128 * side : 128 * side + 128]
                lead = p - q
                lead_ref[lane, at, :] = lead
                force = weighted(lead, own_ref[1, at, :], own_ref[2, at, :], spread)
                here = (own_ref[0, at, :] * keep) * here + force
                force = weighted(p + q, next_ref[1, at, :], next_ref[2, at, :], spread)
                there = (next_ref[0, at, :] * keep) * there + force
            states[side] = (keep, keep_run, spread, here, there)
            if piece < pieces - 1:
                continue
            here, _ = over_runs(here, ends_ref[0] * keep_run)
            there, _ = over_runs(there, ends_ref[1] * keep_run)
            a_ref[pl.ds(lane, 1), :] = here[7:8, :]
            c_ref[pl.ds(lane, 1), :] = there[7:8, :]

    def tail_scan(i, tail):
        for side in range(2):
            lane = 2 * i + side
            keep, keep_run, spread = rate_rows(lane)
            there = jnp.zeros((8, 128), F32)
            for j in range(runs):
                at = slice(8 * j, 8 * j + 8)
                force = weighted(tail(at, slice(128 * side, 128 * side + 128)), next_ref[1, at, :], next_ref[2, at, :], spread)
                there = (next_ref[0, at, :] * keep) * there + force
            there, _ = over_runs(there, ends_ref[1] * keep_run)
            c_ref[pl.ds(lane, 1), :] = there[7:8, :]

    def whole(scan, i, slot):
        scan(i, slot, [None, None], 0, 1)

    def step(i, slot, data, inverse, scan, folding=None):
        states = [None, None]
        for part in range(4):
            forward(data, 1 - slot, part)
            scan((i + chunks - 1) % chunks, 1 - slot, states, part, 8)
            if folding is not None:
                fold(e_ref, es_ref, folding, length, part, 4)
        for part in range(4):
            inverse(slot, part)
            scale(i + 1, 1 - slot, part)
            scan((i + chunks - 1) % chunks, 1 - slot, states, part + 4, 8)
            if folding is not None:
                fold(e_ref, es_ref, folding + 1, length, part, 4)

    def early_step(i, slot, folding=None):
        step(i, slot, doubled(v_ref, i + 1), early_inverse, early_scan, folding)

    first_data = doubled(v_ref, 0)
    for part in range(4):
        forward(first_data, 0, part)
        scale(0, 0, part)
    arrived(inverse_ref, t_sem.at[3])
    def early_pair(u, carry):
        arrived(e_ref.at[pl.ds(pl.multiple_of(4 * u + 4, 4), 4)], e_sem.at[u + 1])

        @pl.when(u == 0)
        def _():
            for lane in range(8, lanes):
                table(lane).start()

        early_step(2 * u, 0, 4 * u + 4)

        early_step(2 * u + 1, 1, 4 * u + 6)

        pl.when((u == 0) & (chip < chips // 2))(meet)

        @pl.when(u < 2)
        def _():
            noise(4 + u).start()

        @pl.when(u == 0)
        def _():
            for slot in range(2):
                tails_ref[slot] = ps[slot][...] + qs[slot][...]

        @pl.when(u == 1)
        def _():
            burst_copy.wait()
            ends_ref[1] = broadcasts(next_burst_ref, next_ref)
            for k in range(2):
                tail_scan(k, lambda at, cut: tails_ref[k, at, cut])
            tail_scan(2, lambda at, cut: ps[0][at, cut] + qs[0][at, cut])

        return carry

    lax.fori_loop(0, chunks // 2 - 1, early_pair, 0)
    early_step(chunks - 2, 0)
    states = [None, None]
    for part in range(4):
        early_inverse(1, part)
        early_scan(chunks - 2, 0, states, part, 4)
    whole(early_scan, chunks - 1, 1)
    sent_early = chunks // 2 + 2

    own_half = pl.ds(pl.multiple_of(core * 8, 8), 8)
    other_half = pl.ds(pl.multiple_of((1 - core) * 8, 8), 8)
    pair_copy = remote(pair_out_ref, pair_in_ref, pair_sem.at[0], pair_sem.at[1], partner)
    give_copy = remote(give_ref, take_ref, give_sem.at[0], give_sem.at[1], partner)
    pair_out_ref[0] = a_ref[other_half, :]
    pair_out_ref[1] = c_ref[other_half, :]
    pair_copy.start()

    for k in range(2):
        arrived(member_logs_ref.at[pl.ds(0, MEMBERS - 1)], logs_sem.at[k])
    member_logs_ref[pl.ds(member, 1)] = logs_ref[...].reshape(1, 1, 128)
    logs_of = [member_logs_ref[k] for k in range(MEMBERS)]
    group_log_ref[0:1, :] = sum(logs_of[1:], logs_of[0])
    group_log_ref[1:2, :] = logs_of[0]
    group_logs_ref[pl.ds(group, 1)] = group_log_ref[...].reshape(1, 2, 128)
    for device in group_peers:
        remote(group_log_ref, group_logs_ref.at[group], glogs_sem.at[0], glogs_sem.at[1], device).start()

    def log_of(index):
        return jnp.broadcast_to(member_logs_ref[index], (8, 128)) - length * rate_ref[own_half, :]

    def of_first(k):
        own = (a_ref, c_ref)[k][own_half, :]
        return jnp.where(core == 0, own, pair_in_ref[k])

    def of_second(k):
        own = (a_ref, c_ref)[k][own_half, :]
        return jnp.where(core == 0, pair_in_ref[k], own)

    def exchange_chips():
        pair_copy.wait()
        chip_out_ref[0] = jnp.exp(log_of(2 * chip + 1)) * of_first(0) + of_first(1) + of_second(0)
        chip_out_ref[1] = of_second(1)
        for device in chip_peers:
            remote(chip_out_ref, chips_ref.at[chip], chips_sem.at[0], chips_sem.at[1], device).start()
        chips_ref[pl.ds(chip, 1)] = chip_out_ref[...].reshape(1, 2, 8, 128)

    def exchange_groups():
        for k in range(2):
            arrived(chips_ref.at[pl.ds(0, chips - 1)], chips_sem.at[k])
        state = jnp.zeros((8, 128), F32)
        log, tail = state, state
        before = (state, log, tail)
        for k in range(chips):
            here = chip == k
            before = tuple(jnp.where(here, new, old) for new, old in zip((state, log, tail), before))
            second = log_of(2 * k + 1)
            step = log_of(2 * k) + second
            state = jnp.exp(step) * state + jnp.exp(second) * tail + chips_ref[k, 0]
            tail = chips_ref[k, 1]
            log = log + step
        group_out_ref[0] = state
        group_out_ref[1] = tail
        for device in group_peers:
            remote(group_out_ref, groups_ref.at[group], groups_sem.at[0], groups_sem.at[1], device).start()
        groups_ref[pl.ds(group, 1)] = group_out_ref[...].reshape(1, 2, 8, 128)
        for k in range(3):
            before_ref[k] = before[k]

    def exchange_back():
        for k in range(2):
            arrived(groups_ref.at[pl.ds(0, groups - 1)], groups_sem.at[k])
        for k in range(2):
            arrived(group_logs_ref.at[pl.ds(0, groups - 1)], glogs_sem.at[k])
        rate = rate_ref[own_half, :]
        entering = groups_ref[(group + groups - 1) % groups, 1]
        state = jnp.zeros((8, 128), F32)
        log, tail = state, entering
        for k in range(groups):
            at = (group + k) % groups
            total = jnp.broadcast_to(group_logs_ref[at, 0:1, :], (8, 128))
            first = jnp.broadcast_to(group_logs_ref[at, 1:2, :], (8, 128))
            step = total - (MEMBERS * length) * rate
            rest = (total - first) - ((MEMBERS - 1) * length) * rate
            state = jnp.exp(step) * state + jnp.exp(rest) * tail + groups_ref[at, 0]
            tail = groups_ref[at, 1]
            log = log + step
        opening = state / (1.0 - jnp.exp(log))
        log = before_ref[1]
        arriving = jnp.where(chip == 0, 0.0, jnp.exp(log - log_of(0)) * entering)
        first_in = jnp.exp(log) * opening + before_ref[0] + arriving
        tail = jnp.where(chip == 0, entering, before_ref[2])
        second_in = jnp.exp(log_of(2 * chip)) * first_in + of_first(0) + tail
        incoming_ref[own_half, :] = jnp.where(core == 0, first_in, second_in)
        give_ref[...] = jnp.where(core == 0, second_in, first_in)
        give_copy.start()

    def arrive(i):
        noise(i).wait_recv()

    def late_inverse(slot, part):
        at = slice(half * part, half * part + half)
        if part < 2:
            ps[slot][at, :] = jnp.dot(inverse_ref[at, :], scaleds[slot][...], preferred_element_type=F32)

    def late_scan(i, slot, states, piece, pieces):
        for side in range(2):
            lane = 2 * i + side
            if piece == 0:
                states[side] = rate_rows(lane) + (jnp.zeros((8, 128), F32),)
            keep, keep_run, spread, state = states[side]
            for j in range(runs * piece // pieces, runs * (piece + 1) // pieces):
                at = slice(8 * j, 8 * j + 8)
                series = lead_ref[lane, at, :] + ps[slot][at, 128 * side : 128 * side + 128]
                force = weighted(series, own_ref[1, at, :], own_ref[2, at, :], spread)
                state = (own_ref[0, at, :] * keep) * state + force
                x_ref[lane, at, :] = state
            states[side] = (keep, keep_run, spread, state)
            if piece < pieces - 1:
                continue
            state, decay = over_runs(state, ends_ref[0] * keep_run)
            row = lax.broadcasted_iota(jnp.int32, (8, 128), 0)
            carry_ref[lane] = jnp.where(row == 0, 0.0, pltpu.roll(state, 1, 0))
            reach_ref[lane] = jnp.where(row == 0, 1.0, pltpu.roll(decay, 1, 0))

    def late_step(i, slot):
        step(i, slot, doubled(earlier_ref, i + 1), late_inverse, late_scan)

    arrive(0)
    first_data = doubled(earlier_ref, 0)
    for part in range(4):
        forward(first_data, 0, part)
        scale(0, 0, part)

    def late_pair(u, carry):
        arrive(2 * u + 1)
        late_step(2 * u, 0)

        @pl.when(u == 0)
        def _():
            exchange_chips()
            for i in range(sent_early, chunks):
                noise(i).start()

        arrive(2 * u + 2)
        late_step(2 * u + 1, 1)
        pl.when(u == 1)(exchange_groups)
        return carry

    lax.fori_loop(0, chunks // 2 - 1, late_pair, 0)
    states = [None, None]
    for part in range(2):
        late_inverse(0, part)
        late_scan(chunks - 3, 1, states, part, 2)
    whole(late_scan, chunks - 2, 0)
    arrive(chunks - 1)
    last_data = doubled(earlier_ref, chunks - 1)
    for part in range(4):
        forward(last_data, 1, part)
        scale(chunks - 1, 1, part)
    exchange_back()
    states = [None, None]
    for part in range(2):
        late_inverse(1, part)
    for part in range(2):
        late_scan(chunks - 1, 1, states, part, 2)
    give_copy.wait()
    incoming_ref[other_half, :] = take_ref[...]
    for lane in range(lanes):
        incoming = jnp.broadcast_to(incoming_ref[lane : lane + 1, :], (8, 128))
        x_ref[lane, length : length + 8, :] = carry_ref[lane] + reach_ref[lane] * incoming

    arrived(earlier_ref, noise_send.at[0])


def close(length, x_ref, out_hbm, stage_ref, sem):
    lanes = stage_ref.shape[0]
    runs = length // 8
    spread_ref = stage_ref.reshape(lanes, 8 * (runs + 8), 128)

    def out(lane):
        return pltpu.make_async_copy(
            stage_ref.at[lane, :, pl.ds(0, runs)],
            out_hbm.at[:, :, pl.ds(pl.multiple_of(lane * 128, 128), 128)],
            sem.at[0],
        )

    def step(pair, carry):
        both = (2 * pair, 2 * pair + 1)
        keep = [jnp.exp(-jnp.broadcast_to(x_ref[lanes + 1, pl.ds(lane, 1), :], (8, 128))) for lane in both]
        state = [x_ref[lane, length : length + 8, :] * k for lane, k in zip(both, keep)]
        for j in range(runs):
            at = slice(8 * j, 8 * j + 8)
            grown = x_ref[lanes, at, :]
            for side, lane in enumerate(both):
                spread_ref[lane, pl.ds(j, 8, stride=runs + 8), :] = x_ref[lane, at, :] + grown * state[side]
                state[side] = state[side] * keep[side]
        for lane in both:
            out(lane).start()
        return carry

    lax.fori_loop(0, lanes // 2, step, 0)

    written = stage_ref.at[:, :, pl.ds(0, runs)]
    pltpu.make_async_copy(written, written, sem.at[0]).wait()


def shards(sections, random_forcing, eigen_root_table, lane_fading_speed, sudden_shrink):
    length, width = random_forcing.shape
    lanes, half = width // 128, length // 2
    chunk = 256
    chunks = width // chunk
    groups, chips = sections // MEMBERS, MEMBERS // 2
    forward, inverse = tables(length)
    hbm = pl.BlockSpec(memory_space=pltpu.HBM)
    vmem = pl.BlockSpec(memory_space=pltpu.VMEM)
    dma = pltpu.SemaphoreType.DMA
    tile = pltpu.VMEM((8, 128), F32)
    dense = pltpu.VMEM((lanes, 128), F32)
    x = pl.pallas_call(
        functools.partial(fields, length, sections),
        name="fields",
        out_shape=pltpu.VMEM((lanes + 2, length + 8, 128), F32),
        in_specs=[hbm] * 6,
        out_specs=vmem,
        scratch_shapes=[
            pltpu.VMEM((length, width), BF16),
            pltpu.VMEM((lanes, 2 * length, 128), F32),
            pltpu.VMEM((2 * length, 2 * length), BF16),
            pltpu.VMEM((length, 6 * length), BF16),
            dense,
            pltpu.VMEM((length // 128, 128), F32),
            pltpu.VMEM((lanes, 3 * half, 128), F32),
            pltpu.VMEM((length, width), BF16),
            pltpu.VMEM((2 * length, chunk), BF16),
            pltpu.VMEM((2 * length, chunk), F32),
            pltpu.VMEM((2 * length, chunk), F32),
            pltpu.VMEM((6 * length, chunk), BF16),
            pltpu.VMEM((6 * length, chunk), BF16),
            pltpu.VMEM((length, chunk), F32),
            pltpu.VMEM((length, chunk), F32),
            pltpu.VMEM((length, chunk), F32),
            pltpu.VMEM((length, chunk), F32),
            pltpu.VMEM((2, length, chunk), F32),
            pltpu.VMEM((lanes, length, 128), F32),
            pltpu.VMEM((3, length, 128), F32),
            pltpu.VMEM((3, length, 128), F32),
            tile,
            tile,
            pltpu.VMEM((2, 8, 128), F32),
            pltpu.VMEM((lanes, 8, 128), F32),
            pltpu.VMEM((lanes, 8, 128), F32),
            dense,
            pltpu.VMEM((1, 128), F32),
            dense,
            dense,
            pltpu.VMEM((2, 8, 128), F32),
            pltpu.VMEM((2, 8, 128), F32),
            pltpu.VMEM((3, 8, 128), F32),
            pltpu.VMEM((chips, 2, 8, 128), F32),
            pltpu.VMEM((groups, 2, 8, 128), F32),
            pltpu.VMEM((MEMBERS, 1, 128), F32),
            pltpu.VMEM((groups, 2, 128), F32),
            pltpu.VMEM((2, 128), F32),
            pltpu.VMEM((2, 8, 128), F32),
            pltpu.VMEM((2, 8, 128), F32),
            tile,
            tile,
            dma((5,)),
            dma((lanes // 4,)),
            dma((1,)),
            dma((chunks,)),
        ]
        + [dma((2,))] * 7,
        compiler_params=pltpu.CompilerParams(
            collective_id=0, has_side_effects=True, vmem_limit_bytes=44 * 2**20
        ),
    )(
        *(
            pltpu.with_memory_space_constraint(operand, pltpu.HBM)
            for operand in (
                random_forcing,
                eigen_root_table,
                jnp.asarray(forward),
                jnp.asarray(inverse),
                lane_fading_speed.reshape(lanes, 128),
                sudden_shrink.reshape(length // 128, 128),
            )
        )
    )
    return pl.pallas_call(
        functools.partial(close, length),
        name="close",
        out_shape=jax.ShapeDtypeStruct((8, length // 8, width), F32),
        in_specs=[vmem],
        out_specs=hbm,
        scratch_shapes=[pltpu.VMEM((lanes, 8, length // 8 + 8, 128), F32), dma((1,))],
        compiler_params=pltpu.CompilerParams(vmem_limit_bytes=8 * 2**20),
    )(x).reshape(length, width)


def solution(mesh):
    return jax.shard_map(
        functools.partial(shards, mesh.shape["tm"]),
        mesh=mesh,
        in_specs=(P("tm", "chan"), P(None, "chan"), P("chan"), P("tm")),
        out_specs=P("tm", "chan"),
        check_vma=False,
    )
```
